16 devices in a mesh: rep: 1, dp: 16 (over x, y, z, core).
Axes of the slice: x: 2, y: 2, z: 2, core: 2. Of those that a mesh axis runs over, the one named last changes fastest.
Arguments:
- g_w_gate: bfloat16 [16, 2, 1024, 3072], P(('rep', 'dp'))
- g_w_up: bfloat16 [16, 2, 1024, 3072], P(('rep', 'dp'))
- g_w_down: bfloat16 [16, 2, 3072, 1024], P(('rep', 'dp'))
- w_gate: bfloat16 [2, 1024, 3072], replicated
- w_up: bfloat16 [2, 1024, 3072], replicated
- w_down: bfloat16 [2, 3072, 1024], replicated
- m_w_gate: float32 [2, 1024, 3072], P(None, 'dp')
- m_w_up: float32 [2, 1024, 3072], P(None, 'dp')
- m_w_down: float32 [2, 3072, 1024], P(None, 'dp')
- v_w_gate: float32 [2, 1024, 3072], P(None, 'dp')
- v_w_up: float32 [2, 1024, 3072], P(None, 'dp')
- v_w_down: float32 [2, 3072, 1024], P(None, 'dp')
Outputs:
- output 1: bfloat16 [2, 1024, 3072], P('rep')
- output 2: bfloat16 [2, 1024, 3072], P('rep')
- output 3: bfloat16 [2, 3072, 1024], P('rep')
- output 4: float32 [2, 1024, 3072], P('rep', 'dp')
- output 5: float32 [2, 1024, 3072], P('rep', 'dp')
- output 6: float32 [2, 3072, 1024], P('rep', 'dp')
- output 7: float32 [2, 1024, 3072], P('rep', 'dp')
- output 8: float32 [2, 1024, 3072], P('rep', 'dp')
- output 9: float32 [2, 3072, 1024], P('rep', 'dp')
All inputs are finite; a program needn't handle non-finite values.
Results may differ from the reference program's by a relative error of at most 0.022.
Values are sent between devices in bfloat16 or wider.
A program may use at most 2 GiB of HBM per device.

```python
import jax
import jax.numpy as jnp
from jax import lax

DEVICES = 16
D = 1024
FF = 3072
LAYERS = 2
NAMES = ("w_gate", "w_up", "w_down")
SHAPES = {"w_gate": (LAYERS, D, FF), "w_up": (LAYERS, D, FF), "w_down": (LAYERS, FF, D)}


def setup_inputs(seed: int = 0, part: int = 0) -> dict:
    kz, *keys = jax.random.split(jax.random.key(seed), 1 + 5 * len(NAMES))
    loud = 2.0 ** jax.random.uniform(kz, (), jnp.float32, -1.0, 1.0)
    drawn = {}
    for name, key, both in zip(NAMES, keys[:3], keys[3:6], strict=True):
        own = jax.random.normal(jax.random.fold_in(key, part), (DEVICES, *SHAPES[name]), jnp.float32)
        shared = jax.random.normal(jax.random.fold_in(both, part), SHAPES[name], jnp.float32)
        drawn["g_" + name] = (loud * (0.7 * shared / DEVICES + 0.7 * own * DEVICES**-0.5)).astype(jnp.bfloat16)
    for name, key in zip(NAMES, keys[6:9], strict=True):
        drawn[name] = (jax.random.normal(key, SHAPES[name], jnp.float32) * SHAPES[name][1] ** -0.5).astype(jnp.bfloat16)
    for name, key in zip(NAMES, keys[9:12], strict=True):
        drawn["m_" + name] = loud * 0.5 * jax.random.normal(key, SHAPES[name], jnp.float32)
    for name, key in zip(NAMES, keys[12:15], strict=True):
        drawn["v_" + name] = loud * loud * jax.random.uniform(key, SHAPES[name], jnp.float32, 0.5, 1.5)
    return drawn


def adamw(w, m, v, g):
    m = 0.9 * m + 0.1 * g
    v = 0.95 * v + 0.05 * g * g
    step = m * lax.rsqrt(v + 1e-8) + 0.1 * w
    return (w - 0.02 * step).astype(jnp.bfloat16), m, v


def reference(g_w_gate, g_w_up, g_w_down, w_gate, w_up, w_down, m_w_gate, m_w_up, m_w_down, v_w_gate, v_w_up, v_w_down):
    def total(terms):
        return lax.scan(lambda so_far, term: (so_far + term.astype(jnp.float32), None), jnp.zeros(terms.shape[1:], jnp.float32), terms)[0]

    gradients = [total(terms).astype(jnp.bfloat16).astype(jnp.float32) for terms in (g_w_gate, g_w_up, g_w_down)]
    new = [
        adamw(w.astype(jnp.float32), m, v, g)
        for w, m, v, g in zip((w_gate, w_up, w_down), (m_w_gate, m_w_up, m_w_down), (v_w_gate, v_w_up, v_w_down), gradients, strict=True)
    ]
    return tuple(one[which] for which in range(3) for one in new)
```

```python
import jax
import jax.numpy as jnp
from jax import lax
from jax.experimental import pallas as pl
from jax.experimental.pallas import tpu as pltpu
from jax.sharding import PartitionSpec as P

X, Y, Z = 4, 2, 1
ORDERS = ((X, Y, Z), (Y, Z, X), (Z, X, Y))
LAYERS = 2
HALVES = 2
CHUNKS = tuple((layer, half) for layer in range(LAYERS) for half in range(HALVES))
TILE = 16


def slots(order):
    d1, d2, d3 = order
    kept = [d2 ^ d3, d2, d3, 0]
    return [d1 ^ r for r in kept] + kept


def total(refs):
    acc = refs[0].astype(jnp.float32)
    for one in refs[1:]:
        acc = acc + one.astype(jnp.float32)
    return acc


def kernel(*refs):
    g, w, m, v, out_w, out_m, out_v = (refs[i : i + 3] for i in range(0, 21, 3))
    theirs, recv1, recv2, recv3, mine, own_w, own_m, own_v = (refs[i : i + 3] for i in range(21, 45, 3))
    (pair_send, pair_recv, mine_sem, rs_send, rs_recv, state_sem, ag_send, ag_recv, agp_send, agp_recv, wb_sem) = refs[45:]

    me = lax.axis_index("dp")
    core = lax.rem(me, 2)
    bits = {Z: lax.rem(lax.div(me, 2), 2), Y: lax.rem(lax.div(me, 4), 2), X: lax.div(me, 8)}

    def chip(mask):
        return sum(d * ((1 - bits[d]) if mask & d else bits[d]) for d in (X, Y, Z))

    def at(mask):
        return {"dp": chip(mask) * 2 + core}

    partner = {"dp": me + 1 - 2 * core}
    rows_of = [one.shape[1] for one in m]

    def rows(k, mask, which, half):
        size = rows_of[k] // HALVES
        start = (chip(mask) * 2 + which) * rows_of[k] + half * size
        return pl.ds(pl.multiple_of(start, TILE), size)

    def part(k, half):
        size = rows_of[k] // HALVES
        return pl.ds(half * size, size)

    def remote(src, dst, send, recv, device):
        return pltpu.make_async_remote_copy(
            src_ref=src, dst_ref=dst, send_sem=send, recv_sem=recv, device_id=device, device_id_type=pl.DeviceIdType.MESH
        )

    events = [(c, layer, half, k) for c, (layer, half) in enumerate(CHUNKS) for k in range(3)]

    def load_mine(k, c, layer, half, group):
        return [
            pltpu.make_async_copy(g[k].at[layer, rows(k, r, core, half)], mine[k].at[layer, j, part(k, half)], mine_sem.at[group, k, c])
            for j, r in enumerate(slots(ORDERS[k])[4 * group : 4 * group + 4])
        ]

    def pair(k, c, layer, half, group):
        return [
            remote(
                g[k].at[layer, rows(k, r, 1 - core, half)],
                theirs[k].at[layer, 4 * group + j, part(k, half)],
                pair_send.at[group, k, c],
                pair_recv.at[group, k, c],
                partner,
            )
            for j, r in enumerate(slots(ORDERS[k])[4 * group : 4 * group + 4])
        ]

    for c, layer, half, k in events:
        for copy in load_mine(k, c, layer, half, 0):
            copy.start()

    barrier = pltpu.get_barrier_semaphore()
    for peer in (partner, at(X), at(Y), at(Z)):
        pl.semaphore_signal(barrier, inc=1, device_id=peer, device_id_type=pl.DeviceIdType.MESH)
    pl.semaphore_wait(barrier, 4)

    for group in range(2):
        for c, layer, half, k in events:
            for copy in pair(k, c, layer, half, group):
                copy.start()

    def wait_pair(k, c, layer, half, group):
        spot = theirs[k].at[layer, pl.ds(4 * group, 4), part(k, half)]
        remote(spot, spot, pair_send.at[group, k, c], pair_recv.at[group, k, c], partner).wait_recv()

    def wait_mine(k, c, layer, half, group):
        spot = mine[k].at[layer, :, part(k, half)]
        pltpu.make_async_copy(spot, spot, mine_sem.at[group, k, c]).wait()

    def add(k, layer, half, first, count, extra):
        size = rows_of[k] // HALVES
        step = TILE * (1 if k < 2 else 3)

        def body(i, _):
            j = lax.div(i, size // step)
            spot = pl.ds(pl.multiple_of(half * size + lax.rem(i, size // step) * step, TILE), step)
            terms = [theirs[k][layer, first + j, spot], mine[k][layer, lax.rem(first, 4) + j, spot]]
            terms += [one[layer, slot + j, spot] for one, slot in extra]
            theirs[k][layer, first + j, spot] = total(terms).astype(jnp.bfloat16)
            return 0

        lax.fori_loop(0, count * size // step, body, 0)

    def hop(stage, k, c, layer, half):
        src, dst = (
            (theirs[k].at[layer, pl.ds(0, 4)], recv1[k].at[layer]),
            (theirs[k].at[layer, pl.ds(4, 2)], recv2[k].at[layer]),
            (theirs[k].at[layer, pl.ds(6, 1)], recv3[k].at[layer]),
        )[stage]
        return remote(
            src.at[:, part(k, half)], dst.at[:, part(k, half)], rs_send.at[stage, k, c], rs_recv.at[stage, k, c], at(ORDERS[k][stage])
        )

    for c, layer, half, k in events:
        wait_mine(k, c, layer, half, 0)
        wait_pair(k, c, layer, half, 0)
        add(k, layer, half, 0, 4, [])
        hop(0, k, c, layer, half).start()
        for copy in load_mine(k, c, layer, half, 1):
            copy.start()

    def state(k, c, layer, half):
        here = part(k, half)
        return [
            pltpu.make_async_copy(w[k].at[layer, rows(k, 0, core, half)], own_w[k].at[layer, here], state_sem.at[0, k, c]),
            pltpu.make_async_copy(m[k].at[layer, here], own_m[k].at[layer, here], state_sem.at[1, k, c]),
            pltpu.make_async_copy(v[k].at[layer, here], own_v[k].at[layer, here], state_sem.at[2, k, c]),
        ]

    for c, layer, half, k in events:
        for copy in state(k, c, layer, half):
            copy.start()

    for c, layer, half, k in events:
        wait_mine(k, c, layer, half, 1)
        wait_pair(k, c, layer, half, 1)
        hop(0, k, c, layer, half).wait_recv()
        add(k, layer, half, 4, 2, [(recv1[k], 0)])
        hop(1, k, c, layer, half).start()
    for c, layer, half, k in events:
        hop(1, k, c, layer, half).wait_recv()
        add(k, layer, half, 6, 1, [(recv1[k], 2), (recv2[k], 0)])
        hop(2, k, c, layer, half).start()

    def adamw(k, layer, half):
        size = rows_of[k] // HALVES
        step = TILE * (1 if k < 2 else 3)

        def body(i, _):
            spot = pl.ds(pl.multiple_of(half * size + i * step, TILE), step)
            terms = [theirs[k][layer, 7, spot], mine[k][layer, 3, spot], recv1[k][layer, 3, spot], recv2[k][layer, 1, spot], recv3[k][layer, 0, spot]]
            grad = total(terms).astype(jnp.bfloat16).astype(jnp.float32)
            old = own_w[k][layer, spot].astype(jnp.float32)
            new_m = 0.9 * own_m[k][layer, spot] + 0.1 * grad
            new_v = 0.95 * own_v[k][layer, spot] + 0.05 * grad * grad
            own_m[k][layer, spot] = new_m
            own_v[k][layer, spot] = new_v
            own_w[k][layer, spot] = (old - 0.02 * (new_m * lax.rsqrt(new_v + 1e-8) + 0.1 * old)).astype(jnp.bfloat16)
            return 0

        lax.fori_loop(0, size // step, body, 0)

    def gather(k, c, layer, half, src, mask, dim):
        d = ORDERS[k][dim]
        spot = out_w[k].at[layer, rows(k, mask, core, half)]
        return remote(src if src is not None else spot, spot, ag_send.at[k], ag_recv.at[k, c, (mask ^ d) - 1], at(d))

    def wait_gather(k, c, layer, half, mask):
        spot = out_w[k].at[layer, rows(k, mask, core, half)]
        remote(spot, spot, ag_send.at[k], ag_recv.at[k, c, mask - 1], at(X)).wait_recv()

    def to_partner(k, layer, half, src, mask):
        spot = out_w[k].at[layer, rows(k, mask, core, half)]
        return remote(src if src is not None else spot, spot, agp_send.at[k], agp_recv.at[k], partner)

    def write_back(k, layer, half):
        here = part(k, half)
        return [
            pltpu.make_async_copy(own_w[k].at[layer, here], out_w[k].at[layer, rows(k, 0, core, half)], wb_sem.at[0, k]),
            pltpu.make_async_copy(own_m[k].at[layer, here], out_m[k].at[layer, here], wb_sem.at[1, k]),
            pltpu.make_async_copy(own_v[k].at[layer, here], out_v[k].at[layer, here], wb_sem.at[2, k]),
        ]

    for c, layer, half, k in events:
        for copy in state(k, c, layer, half):
            copy.wait()
        hop(2, k, c, layer, half).wait_recv()
        adamw(k, layer, half)
        new = own_w[k].at[layer, part(k, half)]
        for dim in (2, 1, 0):
            gather(k, c, layer, half, new, 0, dim).start()
        to_partner(k, layer, half, new, 0).start()
        for copy in write_back(k, layer, half):
            copy.start()

    for c, layer, half, k in events:
        d1, d2, d3 = ORDERS[k]
        wait_gather(k, c, layer, half, d3)
        for dim in (1, 0):
            gather(k, c, layer, half, None, d3, dim).start()
        to_partner(k, layer, half, None, d3).start()
    for c, layer, half, k in events:
        d1, d2, d3 = ORDERS[k]
        for mask in (d2, d2 ^ d3):
            wait_gather(k, c, layer, half, mask)
            gather(k, c, layer, half, None, mask, 0).start()
            to_partner(k, layer, half, None, mask).start()
    for c, layer, half, k in events:
        d1, d2, d3 = ORDERS[k]
        for mask in (d1, d1 ^ d3, d1 ^ d2, d1 ^ d2 ^ d3):
            wait_gather(k, c, layer, half, mask)
            to_partner(k, layer, half, None, mask).start()

    for c, layer, half, k in events:
        for group in range(2):
            spot = theirs[k].at[layer, pl.ds(4 * group, 4), part(k, half)]
            remote(spot, spot, pair_send.at[group, k, c], pair_recv.at[group, k, c], partner).wait_send()
        for stage in range(3):
            hop(stage, k, c, layer, half).wait_send()
    for k in range(3):
        sent = out_w[k].at[0, pl.ds(0, 14 * rows_of[k])]
        remote(sent, sent, ag_send.at[k], ag_recv.at[k, 0, 0], partner).wait_send()
        whole = out_w[k].at[0]
        remote(whole, whole, agp_send.at[k], agp_recv.at[k], partner).wait()
        pltpu.make_async_copy(own_w[k], own_w[k], wb_sem.at[0, k]).wait()
        pltpu.make_async_copy(own_m[k], own_m[k], wb_sem.at[1, k]).wait()
        pltpu.make_async_copy(own_v[k], own_v[k], wb_sem.at[2, k]).wait()


def solution(mesh):
    def step(*arrays):
        terms = [one.reshape(one.shape[1:]) for one in arrays[:3]]
        weights, m, v = arrays[3:6], arrays[6:9], arrays[9:12]
        blocks = [one.shape[1:] for one in m]
        n = len(CHUNKS)

        def scratch(dtype, *lead):
            return [pltpu.VMEM((LAYERS, *lead, *block), dtype) for block in blocks]

        dma = pltpu.SemaphoreType.DMA
        out = pl.pallas_call(
            kernel,
            out_shape=[jax.ShapeDtypeStruct(one.shape, one.dtype) for one in (*weights, *m, *v)],
            in_specs=[pl.BlockSpec(memory_space=pl.ANY)] * 12,
            out_specs=[pl.BlockSpec(memory_space=pl.ANY)] * 9,
            scratch_shapes=[
                *scratch(jnp.bfloat16, 8),
                *scratch(jnp.bfloat16, 4),
                *scratch(jnp.bfloat16, 2),
                *scratch(jnp.bfloat16, 1),
                *scratch(jnp.bfloat16, 4),
                *scratch(jnp.bfloat16),
                *scratch(jnp.float32),
                *scratch(jnp.float32),
                dma((2, 3, n)),
                dma((2, 3, n)),
                dma((2, 3, n)),
                dma((3, 3, n)),
                dma((3, 3, n)),
                dma((3, 3, n)),
                dma((3,)),
                dma((3, n, 7)),
                dma((3,)),
                dma((3,)),
                dma((3, 3)),
            ],
            compiler_params=pltpu.CompilerParams(collective_id=0, has_side_effects=True, vmem_limit_bytes=60 * 1024 * 1024),
            name="step",
        )(*terms, *weights, *m, *v)
        return tuple(out)

    all_of, cut = P(None, None, None), P(None, "dp", None)
    return jax.shard_map(
        step,
        mesh=mesh,
        in_specs=(P(("rep", "dp"), None, None, None),) * 3 + (all_of,) * 3 + (cut,) * 6,
        out_specs=(P("rep", None, None),) * 3 + (P("rep", "dp", None),) * 6,
        check_vma=False,
    )
```

```python
import jax
import jax.numpy as jnp
from jax import lax
from jax.experimental import pallas as pl
from jax.experimental.pallas import tpu as pltpu
from jax.sharding import PartitionSpec as P

X, Y, Z = 4, 2, 1
ORDERS = ((X, Y, Z), (Y, Z, X), (Z, X, Y))
LAYERS = 2
HALVES = 2
CHUNKS = tuple((layer, half) for layer in range(LAYERS) for half in range(HALVES))
TILE = 16
VMEM = 15 * 512 * 1024
THEIRS, LAND1, LAND2, LAND3, OLD = 0, 8, 12, 14, 15
RING = 12
STAGES = ((0, 4), (4, 2), (6, 1), (7, 1))


def ring():
    order = [(stage, c) for stage in range(4) for c in range(len(CHUNKS))]
    place, then, holder, unit = {}, {}, {}, 0
    for stage, c in order:
        count = STAGES[stage][1]
        place[stage, c] = unit % RING
        blocks = [(unit + i) % RING for i in range(count)]
        before = [holder[b] for b in blocks if b in holder]
        then.setdefault(max(before, key=order.index) if before else None, []).append((stage, c))
        holder.update({b: (stage, c) for b in blocks})
        unit += count
    return place, then


PLACE, THEN = ring()


def slots(order):
    d1, d2, d3 = order
    kept = [d2 ^ d3, d2, d3, 0]
    return [d1 ^ r for r in kept] + kept


def total(refs):
    acc = refs[0].astype(jnp.float32)
    for one in refs[1:]:
        acc = acc + one.astype(jnp.float32)
    return acc


def kernel(*refs):
    g, w, m, v, out_w, out_m, out_v = (refs[i : i + 3] for i in range(0, 21, 3))
    mine = refs[21:24]
    (pair_send, pair_recv, mine_sem, rs_send, rs_recv, state_sem, free, ag_send, ag_recv, agp_send, agp_recv) = refs[24:]

    me = lax.axis_index("dp")
    core = lax.rem(me, 2)
    bits = {Z: lax.rem(lax.div(me, 2), 2), Y: lax.rem(lax.div(me, 4), 2), X: lax.div(me, 8)}

    def chip(mask):
        return sum(d * ((1 - bits[d]) if mask & d else bits[d]) for d in (X, Y, Z))

    def at(mask):
        return {"dp": chip(mask) * 2 + core}

    partner = {"dp": me + 1 - 2 * core}
    peers = (partner, at(X), at(Y), at(Z))
    rows_of = [one.shape[1] for one in m]

    def rows(k, mask, which, half):
        size = rows_of[k] // HALVES
        start = (chip(mask) * 2 + which) * rows_of[k] + half * size
        return pl.ds(pl.multiple_of(start, TILE), size)

    def part(k, half, slot=0):
        size = rows_of[k] // HALVES
        return pl.ds(slot * rows_of[k] + half * size, size)

    def remote(src, dst, send, recv, device):
        return pltpu.make_async_remote_copy(
            src_ref=src, dst_ref=dst, send_sem=send, recv_sem=recv, device_id=device, device_id_type=pl.DeviceIdType.MESH
        )

    events = [(c, layer, half, k) for c, (layer, half) in enumerate(CHUNKS) for k in range(3)]

    def load_mine(k, after):
        for stage, c in THEN.get(after, []):
            layer, half = CHUNKS[c]
            first, count = STAGES[stage]
            for j, r in enumerate(slots(ORDERS[k])[first : first + count]):
                source = g[k].at[layer, rows(k, r, core, half)]
                pltpu.make_async_copy(source, mine[k].at[PLACE[stage, c] + j], mine_sem.at[stage, k, c]).start()

    def pair(k, c, layer, half, group):
        return [
            remote(
                g[k].at[layer, rows(k, r, 1 - core, half)],
                out_w[k].at[layer, part(k, half, THEIRS + 4 * group + j)],
                pair_send.at[group, k, c],
                pair_recv.at[group, k, c],
                partner,
            )
            for j, r in enumerate(slots(ORDERS[k])[4 * group : 4 * group + 4])
        ]

    for k in range(3):
        load_mine(k, None)

    barrier = pltpu.get_barrier_semaphore()
    for peer in peers:
        pl.semaphore_signal(barrier, inc=1, device_id=peer, device_id_type=pl.DeviceIdType.MESH)
    pl.semaphore_wait(barrier, 4)

    for group in range(2):
        for c, layer, half, k in events:
            for copy in pair(k, c, layer, half, group):
                copy.start()

    def pair_all(k, c, layer, half, group):
        spot = mine[k].at[pl.ds(0, 4)]
        return remote(spot, spot, pair_send.at[group, k, c], pair_recv.at[group, k, c], partner)

    def wait_mine(k, c, stage):
        spot = mine[k].at[pl.ds(0, STAGES[stage][1])]
        pltpu.make_async_copy(spot, spot, mine_sem.at[stage, k, c]).wait()

    def step_of(k):
        return TILE * (1 if k < 2 else 3)

    def slot_rows(k, half, slot, i):
        return pl.ds(pl.multiple_of(slot * rows_of[k] + half * (rows_of[k] // HALVES) + i * step_of(k), TILE), step_of(k))

    def add(k, c, layer, half, stage, extra):
        first, count = STAGES[stage]
        steps = rows_of[k] // HALVES // step_of(k)

        def body(n, _):
            j, i = lax.div(n, steps), lax.rem(n, steps)
            here = slot_rows(k, half, THEIRS + first + j, i)
            terms = [out_w[k][layer, here], mine[k][PLACE[stage, c] + j, slot_rows(k, 0, 0, i)]]
            terms += [out_w[k][layer, slot_rows(k, half, slot + j, i)] for slot in extra]
            out_w[k][layer, here] = total(terms).astype(jnp.bfloat16)
            return 0

        wait_mine(k, c, stage)
        lax.fori_loop(0, count * steps, body, 0)
        load_mine(k, (stage, c))

    def hops(stage, k, c, layer, half):
        first, count = STAGES[stage]
        land = (LAND1, LAND2, LAND3)[stage]
        return [
            remote(
                out_w[k].at[layer, part(k, half, THEIRS + first + j)],
                out_w[k].at[layer, part(k, half, land + j)],
                rs_send.at[stage, k, c],
                rs_recv.at[stage, k, c],
                at(ORDERS[k][stage]),
            )
            for j in range(count)
        ]

    def hop_all(stage, k, c, layer, half):
        spot = mine[k].at[pl.ds(0, STAGES[stage][1])]
        return remote(spot, spot, rs_send.at[stage, k, c], rs_recv.at[stage, k, c], partner)

    for c, layer, half, k in events:
        pair_all(k, c, layer, half, 0).wait_recv()
        add(k, c, layer, half, 0, [])
        for copy in hops(0, k, c, layer, half):
            copy.start()

    def state(k, c, layer, half):
        here = part(k, half)
        return [
            pltpu.make_async_copy(w[k].at[layer, rows(k, 0, core, half)], out_w[k].at[layer, part(k, half, OLD)], state_sem.at[0, k, c]),
            pltpu.make_async_copy(m[k].at[layer, here], out_m[k].at[layer, here], state_sem.at[1, k, c]),
            pltpu.make_async_copy(v[k].at[layer, here], out_v[k].at[layer, here], state_sem.at[2, k, c]),
        ]

    for c, layer, half, k in events:
        for copy in state(k, c, layer, half):
            copy.start()

    for c, layer, half, k in events:
        pair_all(k, c, layer, half, 1).wait_recv()
        hop_all(0, k, c, layer, half).wait_recv()
        add(k, c, layer, half, 1, [LAND1])
        for copy in hops(1, k, c, layer, half):
            copy.start()
    for c, layer, half, k in events:
        hop_all(1, k, c, layer, half).wait_recv()
        add(k, c, layer, half, 2, [LAND1 + 2, LAND2])
        for copy in hops(2, k, c, layer, half):
            copy.start()

    def adamw(k, c, layer, half):
        steps = rows_of[k] // HALVES // step_of(k)

        def body(i, _):
            here = slot_rows(k, half, 0, i)
            terms = [out_w[k][layer, slot_rows(k, half, slot, i)] for slot in (THEIRS + 7, LAND1 + 3, LAND2 + 1, LAND3)]
            terms.append(mine[k][PLACE[3, c], slot_rows(k, 0, 0, i)])
            grad = total(terms).astype(jnp.bfloat16).astype(jnp.float32)
            old = out_w[k][layer, slot_rows(k, half, OLD, i)].astype(jnp.float32)
            new_m = 0.9 * out_m[k][layer, here] + 0.1 * grad
            new_v = 0.95 * out_v[k][layer, here] + 0.05 * grad * grad
            out_m[k][layer, here] = new_m
            out_v[k][layer, here] = new_v
            new = old - 0.02 * (new_m * lax.rsqrt(new_v + 1e-8) + 0.1 * old)
            out_w[k][layer, slot_rows(k, half, me, i)] = new.astype(jnp.bfloat16)
            return 0

        wait_mine(k, c, 3)
        lax.fori_loop(0, steps, body, 0)

    def gather(k, c, layer, half, mask, dim):
        d = ORDERS[k][dim]
        spot = out_w[k].at[layer, rows(k, mask, core, half)]
        return remote(spot, spot, ag_send.at[k], ag_recv.at[k, c, (mask ^ d) - 1], at(d))

    def wait_gather(k, c, layer, half, mask):
        spot = out_w[k].at[layer, rows(k, mask, core, half)]
        remote(spot, spot, ag_send.at[k], ag_recv.at[k, c, mask - 1], at(X)).wait_recv()

    def to_partner(k, layer, half, mask):
        spot = out_w[k].at[layer, rows(k, mask, core, half)]
        return remote(spot, spot, agp_send.at[k], agp_recv.at[k], partner)

    def send_own(c, layer, half, k):
        pl.semaphore_wait(free.at[k, c], 4)
        for dim in (2, 1, 0):
            gather(k, c, layer, half, 0, dim).start()
        to_partner(k, layer, half, 0).start()

    for n, (c, layer, half, k) in enumerate(events):
        for copy in state(k, c, layer, half):
            copy.wait()
        hop_all(2, k, c, layer, half).wait_recv()
        for stage in range(3):
            hop_all(stage, k, c, layer, half).wait_send()
        adamw(k, c, layer, half)
        for peer in peers:
            pl.semaphore_signal(free.at[k, c], inc=1, device_id=peer, device_id_type=pl.DeviceIdType.MESH)
        if n:
            send_own(*events[n - 1])
    send_own(*events[-1])

    for c, layer, half, k in events:
        d1, d2, d3 = ORDERS[k]
        wait_gather(k, c, layer, half, d3)
        for dim in (1, 0):
            gather(k, c, layer, half, d3, dim).start()
        to_partner(k, layer, half, d3).start()
    for c, layer, half, k in events:
        d1, d2, d3 = ORDERS[k]
        for mask in (d2, d2 ^ d3):
            wait_gather(k, c, layer, half, mask)
            gather(k, c, layer, half, mask, 0).start()
            to_partner(k, layer, half, mask).start()
    for c, layer, half, k in events:
        d1, d2, d3 = ORDERS[k]
        for mask in (d1, d1 ^ d3, d1 ^ d2, d1 ^ d2 ^ d3):
            wait_gather(k, c, layer, half, mask)
            to_partner(k, layer, half, mask).start()

    for c, layer, half, k in events:
        for group in range(2):
            pair_all(k, c, layer, half, group).wait_send()
    for k in range(3):
        sent = out_w[k].at[0, pl.ds(0, 14 * rows_of[k])]
        remote(sent, sent, ag_send.at[k], ag_recv.at[k, 0, 0], partner).wait_send()
        whole = out_w[k].at[0]
        remote(whole, whole, agp_send.at[k], agp_recv.at[k], partner).wait()


def put_out(*refs):
    sources, targets, sem = refs[:9], refs[9:18], refs[18]
    copies = [pltpu.make_async_copy(a, b, sem.at[i]) for i, (a, b) in enumerate(zip(sources, targets, strict=True))]
    for copy in copies:
        copy.start()
    for copy in copies:
        copy.wait()


def solution(mesh):
    def step(*arrays):
        terms = [one.reshape(one.shape[1:]) for one in arrays[:3]]
        weights, m, v = arrays[3:6], arrays[6:9], arrays[9:12]
        blocks = [one.shape[1:] for one in m]
        n = len(CHUNKS)

        dma = pltpu.SemaphoreType.DMA
        out = pl.pallas_call(
            kernel,
            out_shape=[pltpu.VMEM(one.shape, one.dtype) for one in (*weights, *m, *v)],
            in_specs=[pl.BlockSpec(memory_space=pl.ANY)] * 12,
            out_specs=[pl.BlockSpec(memory_space=pltpu.VMEM)] * 9,
            scratch_shapes=[
                *[pltpu.VMEM((RING, rows // HALVES, columns), jnp.bfloat16) for rows, columns in blocks],
                dma((2, 3, n)),
                dma((2, 3, n)),
                dma((4, 3, n)),
                dma((3, 3, n)),
                dma((3, 3, n)),
                dma((3, 3, n)),
                pltpu.SemaphoreType.REGULAR((3, n)),
                dma((3,)),
                dma((3, n, 7)),
                dma((3,)),
                dma((3,)),
            ],
            compiler_params=pltpu.CompilerParams(collective_id=0, has_side_effects=True, vmem_limit_bytes=VMEM),
            name="step",
        )(*terms, *weights, *m, *v)
        out = pl.pallas_call(
            put_out,
            out_shape=[jax.ShapeDtypeStruct(one.shape, one.dtype) for one in (*weights, *m, *v)],
            in_specs=[pl.BlockSpec(memory_space=pl.ANY)] * 9,
            out_specs=[pl.BlockSpec(memory_space=pl.ANY)] * 9,
            scratch_shapes=[dma((9,))],
            compiler_params=pltpu.CompilerParams(vmem_limit_bytes=VMEM),
            name="put_out",
        )(*out)
        return tuple(out)

    all_of, cut = P(None, None, None), P(None, "dp", None)
    return jax.shard_map(
        step,
        mesh=mesh,
        in_specs=(P(("rep", "dp"), None, None, None),) * 3 + (all_of,) * 3 + (cut,) * 6,
        out_specs=(P("rep", None, None),) * 3 + (P("rep", "dp", None),) * 6,
        check_vma=False,
    )
```

```python
import jax
import jax.numpy as jnp
from jax import lax
from jax.experimental import pallas as pl
from jax.experimental.pallas import tpu as pltpu
from jax.sharding import PartitionSpec as P

X, Y, Z = 4, 2, 1
ORDERS = ((X, Y, Z), (Y, Z, X), (Z, X, Y))
LAYERS = 2
HALVES = 2
CHUNKS = tuple((layer, half) for layer in range(LAYERS) for half in range(HALVES))
TILE = 16
VMEM = 15 * 512 * 1024
THEIRS, LAND1, LAND2, LAND3, OLD = 0, 8, 12, 14, 15
RING = 12
STAGES = ((0, 4), (4, 2), (6, 1), (7, 1))


def ring():
    order = [(stage, c) for stage in range(4) for c in range(len(CHUNKS))]
    place, then, holder, unit = {}, {}, {}, 0
    for stage, c in order:
        count = STAGES[stage][1]
        place[stage, c] = unit % RING
        blocks = [(unit + i) % RING for i in range(count)]
        before = [holder[b] for b in blocks if b in holder]
        then.setdefault(max(before, key=order.index) if before else None, []).append((stage, c))
        holder.update({b: (stage, c) for b in blocks})
        unit += count
    return place, then


PLACE, THEN = ring()
TURN = {0: (0, 1, 1, 0), 1: (1, 1, 1, 1), 2: (0, 0, 0, 0), 3: (1, 1, 1, 1)}
FIRST = {(0, 0): 4, (0, 1): 8, (0, 3): 4, (1, 0): 8, (2, 0): 4, (3, 0): 4}


def slots(order):
    d1, d2, d3 = order
    kept = [d2 ^ d3, d2, d3, 0]
    return [d1 ^ r for r in kept] + kept


def total(refs):
    acc = refs[0].astype(jnp.float32)
    for one in refs[1:]:
        acc = acc + one.astype(jnp.float32)
    return acc


def kernel(*refs):
    g, w, m, v, out_w, out_m, out_v = (refs[i : i + 3] for i in range(0, 21, 3))
    mine = refs[21:24]
    (pair_send, pair_first, pair_recv, pair_kept, mine_sem, rs_send, rs_recv) = refs[24:31]
    (state_sem, free, ag_send, ag_recv, ag_last, agp_send, agp_recv) = refs[31:]

    me = lax.axis_index("dp")
    core = lax.rem(me, 2)
    bits = {Z: lax.rem(lax.div(me, 2), 2), Y: lax.rem(lax.div(me, 4), 2), X: lax.div(me, 8)}

    def chip(mask):
        return sum(d * ((1 - bits[d]) if mask & d else bits[d]) for d in (X, Y, Z))

    def at(mask):
        return {"dp": chip(mask) * 2 + core}

    partner = {"dp": me + 1 - 2 * core}
    peers = (partner, at(X), at(Y), at(Z))
    rows_of = [one.shape[1] for one in m]

    def rows(k, mask, which, half):
        size = rows_of[k] // HALVES
        start = (chip(mask) * 2 + which) * rows_of[k] + half * size
        return pl.ds(pl.multiple_of(start, TILE), size)

    def part(k, half, slot=0):
        size = rows_of[k] // HALVES
        return pl.ds(slot * rows_of[k] + half * size, size)

    def remote(src, dst, send, recv, device):
        return pltpu.make_async_remote_copy(
            src_ref=src, dst_ref=dst, send_sem=send, recv_sem=recv, device_id=device, device_id_type=pl.DeviceIdType.MESH
        )

    events = [(c, layer, half, k) for c, (layer, half) in enumerate(CHUNKS) for k in range(3)]

    def load_mine(k, after):
        for stage, c in THEN.get(after, []):
            layer, half = CHUNKS[c]
            first, count = STAGES[stage]
            for j, r in enumerate(slots(ORDERS[k])[first : first + count]):
                source = g[k].at[layer, rows(k, r, core, half)]
                pltpu.make_async_copy(source, mine[k].at[PLACE[stage, c] + j], mine_sem.at[TURN[stage][c], k]).start()

    def pair(k, c, layer, half, slot):
        r = slots(ORDERS[k])[slot]
        arrived = pair_kept.at[k] if slot > 3 else pair_recv.at[k, c - 1] if c else pair_first.at[k, slot]
        here = out_w[k].at[layer, part(k, half, THEIRS + slot)]
        return remote(g[k].at[layer, rows(k, r, 1 - core, half)], here, pair_send.at[k], arrived, partner)

    for k in range(3):
        load_mine(k, None)

    barrier = pltpu.get_barrier_semaphore()
    for peer in peers:
        pl.semaphore_signal(barrier, inc=1, device_id=peer, device_id_type=pl.DeviceIdType.MESH)
    pl.semaphore_wait(barrier, 4)

    def pair_chunk(c, group):
        for slot in range(4 * group, 4 * group + 4):
            for k in range(3):
                pair(k, c, *CHUNKS[c], slot).start()

    pair_chunk(0, 0)
    pair_chunk(1, 0)

    def arrival(k, blocks, sem):
        spot = out_w[k].at[0, pl.ds(0, blocks * rows_of[k] // HALVES)]
        return remote(spot, spot, pair_send.at[k], sem, partner)

    def departure(k, blocks, sem):
        spot = out_w[k].at[0, pl.ds(0, blocks * rows_of[k] // HALVES)]
        return remote(spot, spot, sem, pair_kept.at[k], partner)

    def wait_mine(k, c, stage):
        if (stage, c) in FIRST:
            spot = mine[k].at[pl.ds(0, FIRST[stage, c])]
            pltpu.make_async_copy(spot, spot, mine_sem.at[TURN[stage][c], k]).wait()

    def step_of(k):
        return TILE * (1 if k < 2 else 3)

    def slot_rows(k, half, slot, i):
        return pl.ds(pl.multiple_of(slot * rows_of[k] + half * (rows_of[k] // HALVES) + i * step_of(k), TILE), step_of(k))

    def add(k, c, layer, half, stage, begin, count, extra):
        first = STAGES[stage][0] + begin
        steps = rows_of[k] // HALVES // step_of(k)

        def body(n, _):
            j, i = lax.div(n, steps), lax.rem(n, steps)
            here = slot_rows(k, half, THEIRS + first + j, i)
            terms = [out_w[k][layer, here], mine[k][PLACE[stage, c] + begin + j, slot_rows(k, 0, 0, i)]]
            terms += [out_w[k][layer, slot_rows(k, half, slot + j, i)] for slot in extra]
            out_w[k][layer, here] = total(terms).astype(jnp.bfloat16)
            return 0

        lax.fori_loop(0, count * steps, body, 0)

    def hop(stage, k, c, layer, half, begin, count):
        first = STAGES[stage][0]
        land = (LAND1, LAND2, LAND3)[stage]
        for j in range(begin, begin + count):
            source = out_w[k].at[layer, part(k, half, THEIRS + first + j)]
            target = out_w[k].at[layer, part(k, half, land + j)]
            remote(source, target, rs_send.at[k, c], rs_recv.at[stage, k, c], at(ORDERS[k][stage])).start()

    for slot in range(4):
        for k in range(3):
            if slot == 0:
                wait_mine(k, 0, 0)
            arrival(k, 1, pair_first.at[k, slot]).wait_recv()
            add(k, 0, *CHUNKS[0], 0, slot, 1, [])
            hop(0, k, 0, *CHUNKS[0], slot, 1)
    for c, group in ((2, 0), (3, 0), (0, 1), (1, 1), (2, 1), (3, 1)):
        pair_chunk(c, group)
    for k in range(3):
        load_mine(k, (0, 0))
    for c, layer, half, k in events[3:]:
        wait_mine(k, c, 0)
        arrival(k, 4, pair_recv.at[k, c - 1]).wait_recv()
        add(k, c, layer, half, 0, 0, 4, [])
        hop(0, k, c, layer, half, 0, 4)
        load_mine(k, (0, c))

    def state(k, c, layer, half):
        here = part(k, half)
        return [
            pltpu.make_async_copy(w[k].at[layer, rows(k, 0, core, half)], out_w[k].at[layer, part(k, half, OLD)], state_sem.at[k]),
            pltpu.make_async_copy(m[k].at[layer, here], out_m[k].at[layer, here], state_sem.at[k]),
            pltpu.make_async_copy(v[k].at[layer, here], out_v[k].at[layer, here], state_sem.at[k]),
        ]

    for c, layer, half, k in events:
        for copy in state(k, c, layer, half):
            copy.start()

    for c, layer, half, k in events:
        if c == 0:
            arrival(k, 4 * len(CHUNKS), pair_kept.at[k]).wait_recv()
        wait_mine(k, c, 1)
        arrival(k, 4, rs_recv.at[0, k, c]).wait_recv()
        add(k, c, layer, half, 1, 0, 2, [LAND1])
        hop(1, k, c, layer, half, 0, 2)
        load_mine(k, (1, c))
    for c, layer, half, k in events:
        wait_mine(k, c, 2)
        arrival(k, 2, rs_recv.at[1, k, c]).wait_recv()
        add(k, c, layer, half, 2, 0, 1, [LAND1 + 2, LAND2])
        hop(2, k, c, layer, half, 0, 1)

    def adamw(k, c, layer, half):
        steps = rows_of[k] // HALVES // step_of(k)

        def body(i, _):
            here = slot_rows(k, half, 0, i)
            terms = [out_w[k][layer, slot_rows(k, half, slot, i)] for slot in (THEIRS + 7, LAND1 + 3, LAND2 + 1, LAND3)]
            terms.append(mine[k][PLACE[3, c], slot_rows(k, 0, 0, i)])
            grad = total(terms).astype(jnp.bfloat16).astype(jnp.float32)
            old = out_w[k][layer, slot_rows(k, half, OLD, i)].astype(jnp.float32)
            new_m = 0.9 * out_m[k][layer, here] + 0.1 * grad
            new_v = 0.95 * out_v[k][layer, here] + 0.05 * grad * grad
            out_m[k][layer, here] = new_m
            out_v[k][layer, here] = new_v
            new = old - 0.02 * (new_m * lax.rsqrt(new_v + 1e-8) + 0.1 * old)
            out_w[k][layer, slot_rows(k, half, me, i)] = new.astype(jnp.bfloat16)
            return 0

        lax.fori_loop(0, steps, body, 0)

    def gathered(k, c, mask):
        d1, d2, d3 = ORDERS[k]
        if not mask & d1:
            return rs_recv.at[(d3, d2, d2 ^ d3).index(mask), k, c]
        return ag_last.at[k, (d1, d1 ^ d3, d1 ^ d2, d1 ^ d2 ^ d3).index(mask)] if c == len(CHUNKS) - 1 else ag_recv.at[k, c]

    def gather(k, c, layer, half, mask, dim):
        d = ORDERS[k][dim]
        spot = out_w[k].at[layer, rows(k, mask, core, half)]
        return remote(spot, spot, ag_send.at[k], gathered(k, c, mask ^ d), at(d))

    def wait_gather(k, c, mask):
        arrival(k, 1, gathered(k, c, mask)).wait_recv()

    def to_partner(k, layer, half, mask):
        spot = out_w[k].at[layer, rows(k, mask, core, half)]
        return remote(spot, spot, agp_send.at[k], agp_recv.at[k], partner)

    def send_own(c, layer, half, k):
        pl.semaphore_wait(free.at[k, c], 4)
        for dim in (2, 1, 0):
            gather(k, c, layer, half, 0, dim).start()
        to_partner(k, layer, half, 0).start()

    for n, (c, layer, half, k) in enumerate(events):
        if c == 0:
            held = out_w[k].at[0, pl.ds(0, 10 * rows_of[k])]
            pltpu.make_async_copy(held, held, state_sem.at[k]).wait()
        wait_mine(k, c, 3)
        arrival(k, 1, rs_recv.at[2, k, c]).wait_recv()
        departure(k, 7, rs_send.at[k, c]).wait_send()
        adamw(k, c, layer, half)
        for peer in peers:
            pl.semaphore_signal(free.at[k, c], inc=1, device_id=peer, device_id_type=pl.DeviceIdType.MESH)
        if n:
            send_own(*events[n - 1])
    send_own(*events[-1])

    for c, layer, half, k in events:
        d1, d2, d3 = ORDERS[k]
        wait_gather(k, c, d3)
        for dim in (1, 0):
            gather(k, c, layer, half, d3, dim).start()
        to_partner(k, layer, half, d3).start()
    for c, (layer, half) in enumerate(CHUNKS):
        for far in range(2):
            for k, (d1, d2, d3) in enumerate(ORDERS):
                mask = d2 ^ d3 * far
                wait_gather(k, c, mask)
                gather(k, c, layer, half, mask, 0).start()
                to_partner(k, layer, half, mask).start()
    for c, (layer, half) in enumerate(CHUNKS):
        for which in range(4):
            for k, (d1, d2, d3) in enumerate(ORDERS):
                if c == len(CHUNKS) - 1:
                    wait_gather(k, c, d1 ^ (0, d3, d2, d2 ^ d3)[which])
                elif which == 0:
                    arrival(k, 4, ag_recv.at[k, c]).wait_recv()
                to_partner(k, layer, half, d1 ^ (0, d3, d2, d2 ^ d3)[which]).start()

    n = len(CHUNKS)
    for k in range(3):
        departure(k, 8 * n, pair_send.at[k]).wait_send()
        departure(k, 7 * n, ag_send.at[k]).wait_send()
        departure(k, 8 * n, agp_send.at[k]).wait_send()
        arrival(k, 8 * n, agp_recv.at[k]).wait_recv()


def put_out(*refs):
    sources, targets, sem = refs[:9], refs[9:18], refs[18]
    copies = [pltpu.make_async_copy(a, b, sem.at[i]) for i, (a, b) in enumerate(zip(sources, targets, strict=True))]
    for copy in copies:
        copy.start()
    for copy in copies:
        copy.wait()


def solution(mesh):
    def step(*arrays):
        terms = [one.reshape(one.shape[1:]) for one in arrays[:3]]
        weights, m, v = arrays[3:6], arrays[6:9], arrays[9:12]
        blocks = [one.shape[1:] for one in m]
        n = len(CHUNKS)

        dma = pltpu.SemaphoreType.DMA
        out = pl.pallas_call(
            kernel,
            out_shape=[pltpu.VMEM(one.shape, one.dtype) for one in (*weights, *m, *v)],
            in_specs=[pl.BlockSpec(memory_space=pl.ANY)] * 12,
            out_specs=[pl.BlockSpec(memory_space=pltpu.VMEM)] * 9,
            scratch_shapes=[
                *[pltpu.VMEM((RING, rows // HALVES, columns), jnp.bfloat16) for rows, columns in blocks],
                dma((3,)),
                dma((3, 4)),
                dma((3, n - 1)),
                dma((3,)),
                dma((2, 3)),
                dma((3, n)),
                dma((3, 3, n)),
                dma((3,)),
                pltpu.SemaphoreType.REGULAR((3, n)),
                dma((3,)),
                dma((3, n - 1)),
                dma((3, 4)),
                dma((3,)),
                dma((3,)),
            ],
            compiler_params=pltpu.CompilerParams(collective_id=0, has_side_effects=True, vmem_limit_bytes=VMEM),
            name="step",
        )(*terms, *weights, *m, *v)
        out = pl.pallas_call(
            put_out,
            out_shape=[jax.ShapeDtypeStruct(one.shape, one.dtype) for one in (*weights, *m, *v)],
            in_specs=[pl.BlockSpec(memory_space=pl.ANY)] * 9,
            out_specs=[pl.BlockSpec(memory_space=pl.ANY)] * 9,
            scratch_shapes=[dma((9,))],
            compiler_params=pltpu.CompilerParams(vmem_limit_bytes=VMEM),
            name="put_out",
        )(*out)
        return tuple(out)

    all_of, cut = P(None, None, None), P(None, "dp", None)
    return jax.shard_map(
        step,
        mesh=mesh,
        in_specs=(P(("rep", "dp"), None, None, None),) * 3 + (all_of,) * 3 + (cut,) * 6,
        out_specs=(P("rep", None, None),) * 3 + (P("rep", "dp", None),) * 6,
        check_vma=False,
    )
```

```python
import functools

import jax
import jax.numpy as jnp
from jax import lax
from jax.experimental import pallas as pl
from jax.experimental.pallas import tpu as pltpu
from jax.sharding import PartitionSpec as P


X, Y, Z = 4, 2, 1
ORDERS = ((X, Y, Z), (Y, Z, X), (Z, X, Y))
LAYERS = 2
HALVES = 2
CHUNKS = tuple((layer, half) for layer in range(LAYERS) for half in range(HALVES))
LAST = len(CHUNKS) - 1
TILE = 16
VMEM = 15 * 512 * 1024
THEIRS, LAND1, LAND2, LAND3, OLD = 0, 8, 12, 14, 15
RING = 12
STAGES = ((0, 4), (4, 2), (6, 1), (7, 1))


def ring():
    order = [(stage, c) for stage in range(4) for c in range(len(CHUNKS))]
    place, then, holder, unit = {}, {}, {}, 0
    for stage, c in order:
        count = STAGES[stage][1]
        place[stage, c] = unit % RING
        blocks = [(unit + i) % RING for i in range(count)]
        before = [holder[b] for b in blocks if b in holder]
        then.setdefault(max(before, key=order.index) if before else None, []).append((stage, c))
        holder.update({b: (stage, c) for b in blocks})
        unit += count
    return place, then


PLACE, THEN = ring()
TURN = {0: (0, 1, 1, 0), 1: (1, 1, 1, 1), 2: (0, 0, 0, 0), 3: (1, 1, 1, 1)}
FIRST = {(0, 0): 4, (0, 1): 8, (0, 3): 4, (1, 0): 8, (2, 0): 4, (3, 0): 4}


def slots(order):
    d1, d2, d3 = order
    kept = [d2 ^ d3, d2, d3, 0]
    return [d1 ^ r for r in kept] + kept


def total(refs):
    acc = refs[0].astype(jnp.float32)
    for one in refs[1:]:
        acc = acc + one.astype(jnp.float32)
    return acc


def kernel(*refs):
    g, w, m, v, out_w, out_m, out_v, later, mine = (refs[i : i + 3] for i in range(0, 27, 3))
    (pair_send, pair_first, pair_recv, pair_kept, mine_sem, rs_send, rs_recv) = refs[27:34]
    (state_sem, free, ag_send, agp_send) = refs[34:]

    me = lax.axis_index("dp")
    core = lax.rem(me, 2)
    bits = {Z: lax.rem(lax.div(me, 2), 2), Y: lax.rem(lax.div(me, 4), 2), X: lax.div(me, 8)}

    def chip(mask):
        return sum(d * ((1 - bits[d]) if mask & d else bits[d]) for d in (X, Y, Z))

    def at(mask):
        return {"dp": chip(mask) * 2 + core}

    partner = {"dp": me + 1 - 2 * core}
    peers = (partner, at(X), at(Y), at(Z))
    rows_of = [one.shape[1] for one in m]

    def rows(k, mask, which, half):
        size = rows_of[k] // HALVES
        start = (chip(mask) * 2 + which) * rows_of[k] + half * size
        return pl.ds(pl.multiple_of(start, TILE), size)

    def part(k, half, slot=0):
        size = rows_of[k] // HALVES
        return pl.ds(slot * rows_of[k] + half * size, size)

    def remote(src, dst, send, recv, device):
        return pltpu.make_async_remote_copy(
            src_ref=src, dst_ref=dst, send_sem=send, recv_sem=recv, device_id=device, device_id_type=pl.DeviceIdType.MESH
        )

    events = [(c, layer, half, k) for c, (layer, half) in enumerate(CHUNKS) for k in range(3)]

    def load_mine(k, after):
        for stage, c in THEN.get(after, []):
            layer, half = CHUNKS[c]
            first, count = STAGES[stage]
            for j, r in enumerate(slots(ORDERS[k])[first : first + count]):
                source = g[k].at[layer, rows(k, r, core, half)]
                pltpu.make_async_copy(source, mine[k].at[PLACE[stage, c] + j], mine_sem.at[TURN[stage][c], k]).start()

    def pair(k, c, layer, half, slot):
        r = slots(ORDERS[k])[slot]
        arrived = pair_kept.at[k] if slot > 3 else pair_recv.at[k, c - 1] if c else pair_first.at[k, slot]
        here = out_w[k].at[layer, part(k, half, THEIRS + slot)]
        return remote(g[k].at[layer, rows(k, r, 1 - core, half)], here, pair_send.at[k], arrived, partner)

    for k in range(3):
        load_mine(k, None)

    barrier = pltpu.get_barrier_semaphore()
    for peer in peers:
        pl.semaphore_signal(barrier, inc=1, device_id=peer, device_id_type=pl.DeviceIdType.MESH)
    pl.semaphore_wait(barrier, 4)

    def pair_chunk(c, group):
        for slot in range(4 * group, 4 * group + 4):
            for k in range(3):
                pair(k, c, *CHUNKS[c], slot).start()

    pair_chunk(0, 0)
    pair_chunk(1, 0)

    def arrival(k, blocks, sem):
        spot = out_w[k].at[0, pl.ds(0, blocks * rows_of[k] // HALVES)]
        return remote(spot, spot, pair_send.at[k], sem, partner)

    def departure(k, blocks, sem):
        spot = out_w[k].at[0, pl.ds(0, blocks * rows_of[k] // HALVES)]
        return remote(spot, spot, sem, pair_kept.at[k], partner)

    def wait_mine(k, c, stage):
        if (stage, c) in FIRST:
            spot = mine[k].at[pl.ds(0, FIRST[stage, c])]
            pltpu.make_async_copy(spot, spot, mine_sem.at[TURN[stage][c], k]).wait()

    def step_of(k):
        return TILE * (1 if k < 2 else 3)

    def slot_rows(k, half, slot, i):
        return pl.ds(pl.multiple_of(slot * rows_of[k] + half * (rows_of[k] // HALVES) + i * step_of(k), TILE), step_of(k))

    def add(k, c, layer, half, stage, begin, count, extra):
        first = STAGES[stage][0] + begin
        steps = rows_of[k] // HALVES // step_of(k)

        def body(n, _):
            j, i = lax.div(n, steps), lax.rem(n, steps)
            here = slot_rows(k, half, THEIRS + first + j, i)
            terms = [out_w[k][layer, here], mine[k][PLACE[stage, c] + begin + j, slot_rows(k, 0, 0, i)]]
            terms += [out_w[k][layer, slot_rows(k, half, slot + j, i)] for slot in extra]
            out_w[k][layer, here] = total(terms).astype(jnp.bfloat16)
            return 0

        lax.fori_loop(0, count * steps, body, 0)

    def hop(stage, k, c, layer, half, begin, count):
        first = STAGES[stage][0]
        land = (LAND1, LAND2, LAND3)[stage]
        for j in range(begin, begin + count):
            source = out_w[k].at[layer, part(k, half, THEIRS + first + j)]
            target = out_w[k].at[layer, part(k, half, land + j)]
            remote(source, target, rs_send.at[k, c], rs_recv.at[stage, k, c], at(ORDERS[k][stage])).start()

    for slot in range(4):
        for k in range(3):
            if slot == 0:
                wait_mine(k, 0, 0)
            arrival(k, 1, pair_first.at[k, slot]).wait_recv()
            add(k, 0, *CHUNKS[0], 0, slot, 1, [])
            hop(0, k, 0, *CHUNKS[0], slot, 1)
    for c, group in ((2, 0), (3, 0), (0, 1), (1, 1), (2, 1), (3, 1)):
        pair_chunk(c, group)
    for k in range(3):
        load_mine(k, (0, 0))
    for c, layer, half, k in events[3:]:
        wait_mine(k, c, 0)
        arrival(k, 4, pair_recv.at[k, c - 1]).wait_recv()
        add(k, c, layer, half, 0, 0, 4, [])
        hop(0, k, c, layer, half, 0, 4)
        load_mine(k, (0, c))

    def state(k, layer, half):
        here = part(k, half)
        return [
            pltpu.make_async_copy(w[k].at[layer, rows(k, 0, core, half)], out_w[k].at[layer, part(k, half, OLD)], state_sem.at[k]),
            pltpu.make_async_copy(m[k].at[layer, here], out_m[k].at[layer, here], state_sem.at[k]),
            pltpu.make_async_copy(v[k].at[layer, here], out_v[k].at[layer, here], state_sem.at[k]),
        ]

    for c, layer, half, k in events:
        for copy in state(k, layer, half):
            copy.start()

    for c, layer, half, k in events:
        if c == 0:
            arrival(k, 4 * len(CHUNKS), pair_kept.at[k]).wait_recv()
        wait_mine(k, c, 1)
        arrival(k, 4, rs_recv.at[0, k, c]).wait_recv()
        add(k, c, layer, half, 1, 0, 2, [LAND1])
        hop(1, k, c, layer, half, 0, 2)
        load_mine(k, (1, c))
    for c, layer, half, k in events:
        wait_mine(k, c, 2)
        arrival(k, 2, rs_recv.at[1, k, c]).wait_recv()
        add(k, c, layer, half, 2, 0, 1, [LAND1 + 2, LAND2])
        hop(2, k, c, layer, half, 0, 1)

    def adamw(k, c, layer, half):
        steps = rows_of[k] // HALVES // step_of(k)

        def body(i, _):
            here = slot_rows(k, half, 0, i)
            terms = [out_w[k][layer, slot_rows(k, half, slot, i)] for slot in (THEIRS + 7, LAND1 + 3, LAND2 + 1, LAND3)]
            terms.append(mine[k][PLACE[3, c], slot_rows(k, 0, 0, i)])
            grad = total(terms).astype(jnp.bfloat16).astype(jnp.float32)
            old = out_w[k][layer, slot_rows(k, half, OLD, i)].astype(jnp.float32)
            new_m = 0.9 * out_m[k][layer, here] + 0.1 * grad
            new_v = 0.95 * out_v[k][layer, here] + 0.05 * grad * grad
            out_m[k][layer, here] = new_m
            out_v[k][layer, here] = new_v
            new = old - 0.02 * (new_m * lax.rsqrt(new_v + 1e-8) + 0.1 * old)
            out_w[k][layer, slot_rows(k, half, me, i)] = new.astype(jnp.bfloat16)
            return 0

        lax.fori_loop(0, steps, body, 0)

    def gathered(k, c, mask):
        d1, d2, d3 = ORDERS[k]
        if not mask & d1:
            return rs_recv.at[(d3, d2, d2 ^ d3).index(mask), k, c]
        return pair_first.at[k, (0, d3, d2, d2 ^ d3).index(mask ^ d1)] if c == LAST - 1 else pair_recv.at[k, c]

    def set_aside(k, layer, half, mask, place):
        start = (chip(mask) * 2 + core) * rows_of[k] + half * (rows_of[k] // HALVES)

        def body(i, _):
            there = pl.ds(pl.multiple_of(start + i * step_of(k), TILE), step_of(k))
            later[k][place, slot_rows(k, 0, 0, i)] = out_w[k][layer, there]
            return 0

        lax.fori_loop(0, rows_of[k] // HALVES // step_of(k), body, 0)

    def gather(k, c, layer, half, mask, dim):
        _, d2, d3 = ORDERS[k]
        d = ORDERS[k][dim]
        spot = out_w[k].at[layer, rows(k, mask, core, half)]
        if dim == 0 and c == LAST:
            set_aside(k, layer, half, mask, (0, d3, d2, d2 ^ d3).index(mask))
        else:
            remote(spot, spot, ag_send.at[k], gathered(k, c, mask ^ d), at(d)).start()

    def wait_gather(k, c, mask):
        arrival(k, 1, gathered(k, c, mask)).wait_recv()

    def to_partner(k, layer, half, mask):
        spot = out_w[k].at[layer, rows(k, mask, core, half)]
        return remote(spot, spot, agp_send.at[k], pair_kept.at[k], partner)

    def send_own(c, layer, half, k):
        pl.semaphore_wait(free.at[k, c], 4)
        for dim in (2, 1, 0):
            gather(k, c, layer, half, 0, dim)
        to_partner(k, layer, half, 0).start()

    for n, (c, layer, half, k) in enumerate(events):
        if c == 0:
            held = out_w[k].at[0, pl.ds(0, 10 * rows_of[k])]
            pltpu.make_async_copy(held, held, state_sem.at[k]).wait()
        wait_mine(k, c, 3)
        arrival(k, 1, rs_recv.at[2, k, c]).wait_recv()
        departure(k, 7, rs_send.at[k, c]).wait_send()
        adamw(k, c, layer, half)
        for peer in peers:
            pl.semaphore_signal(free.at[k, c], inc=1, device_id=peer, device_id_type=pl.DeviceIdType.MESH)
        if n:
            send_own(*events[n - 1])
    send_own(*events[-1])

    for c, layer, half, k in events:
        d1, d2, d3 = ORDERS[k]
        wait_gather(k, c, d3)
        for dim in (1, 0):
            gather(k, c, layer, half, d3, dim)
        to_partner(k, layer, half, d3).start()
    for c, (layer, half) in enumerate(CHUNKS):
        for far in range(2):
            for k, (d1, d2, d3) in enumerate(ORDERS):
                mask = d2 ^ d3 * far
                wait_gather(k, c, mask)
                gather(k, c, layer, half, mask, 0)
                to_partner(k, layer, half, mask).start()
    for c, (layer, half) in enumerate(CHUNKS[:LAST]):
        for which in range(4):
            for k, (d1, d2, d3) in enumerate(ORDERS):
                if c == LAST - 1:
                    arrival(k, 1, pair_first.at[k, which]).wait_recv()
                elif which == 0:
                    arrival(k, 4, pair_recv.at[k, c]).wait_recv()
                to_partner(k, layer, half, d1 ^ (0, d3, d2, d2 ^ d3)[which]).start()

    n = len(CHUNKS)
    for k in range(3):
        departure(k, 8 * n, pair_send.at[k]).wait_send()
        departure(k, 7 * n - 4, ag_send.at[k]).wait_send()
        departure(k, 8 * n - 4, agp_send.at[k]).wait_send()
        arrival(k, 8 * n - 4, pair_kept.at[k]).wait_recv()


def put_out(*refs):
    sources, targets, sem = refs[:9], refs[9:18], refs[18]
    for i, (source, target) in enumerate(zip(sources, targets, strict=True)):
        for layer in range(LAYERS):
            for j in range(4):
                here = pl.ds(j * (source.shape[1] // 4), source.shape[1] // 4)
                pltpu.make_async_copy(source.at[layer, here], target.at[layer, here], sem.at[i]).start()
    for i, (source, target) in enumerate(zip(sources, targets, strict=True)):
        pltpu.make_async_copy(source, target, sem.at[i]).wait()


def put_rest(items, *refs):
    n = len(items)
    sources, out_w, sem = refs[:n], refs[n + 3 : n + 6], refs[n + 6]
    me = lax.axis_index("dp")
    core = lax.rem(me, 2)
    bits = {Z: lax.rem(lax.div(me, 2), 2), Y: lax.rem(lax.div(me, 4), 2), X: lax.div(me, 8)}
    layer, half = CHUNKS[LAST]
    for i, (k, whose) in enumerate(items):
        d1, d2, d3 = ORDERS[k]
        size = sources[i].shape[1]
        for j, r in enumerate((0, d3, d2, d2 ^ d3)):
            chip = sum(d * ((1 - bits[d]) if (d1 ^ r) & d else bits[d]) for d in (X, Y, Z))
            which = 1 - core if whose else core
            start = ((chip * 2 + which) * HALVES + half) * size
            target = out_w[k].at[layer, pl.ds(pl.multiple_of(start, TILE), size)]
            pltpu.make_async_copy(sources[i].at[j], target, sem.at[i]).start()
    for i in range(n):
        pltpu.make_async_copy(sources[i], sources[i], sem.at[i]).wait()


def solution(mesh):
    def step(*arrays):
        terms = [one.reshape(one.shape[1:]) for one in arrays[:3]]
        weights, m, v = arrays[3:6], arrays[6:9], arrays[9:12]
        blocks = [one.shape[1:] for one in m]
        n = len(CHUNKS)

        dma = pltpu.SemaphoreType.DMA
        out = pl.pallas_call(
            kernel,
            out_shape=[pltpu.VMEM(one.shape, one.dtype) for one in (*weights, *m, *v)]
            + [pltpu.VMEM((4, rows // HALVES, columns), jnp.bfloat16) for rows, columns in blocks],
            in_specs=[pl.BlockSpec(memory_space=pl.ANY)] * 12,
            out_specs=[pl.BlockSpec(memory_space=pltpu.VMEM)] * 12,
            scratch_shapes=[
                *[pltpu.VMEM((RING, rows // HALVES, columns), jnp.bfloat16) for rows, columns in blocks],
                dma((3,)),
                dma((3, 4)),
                dma((3, n - 1)),
                dma((3,)),
                dma((2, 3)),
                dma((3, n)),
                dma((3, 3, n)),
                dma((3,)),
                pltpu.SemaphoreType.REGULAR((3, n)),
                dma((3,)),
                dma((3,)),
            ],
            compiler_params=pltpu.CompilerParams(collective_id=0, has_side_effects=True, vmem_limit_bytes=VMEM),
            name="step",
        )(*terms, *weights, *m, *v)
        out, later = out[:9], out[9:]
        own = []
        for k in range(3):
            own.append(lax.ppermute(later[k], "dp", [(i, i ^ 2 * ORDERS[k][0]) for i in range(16)]))
        out = pl.pallas_call(
            put_out,
            out_shape=[jax.ShapeDtypeStruct(one.shape, one.dtype) for one in (*weights, *m, *v)],
            in_specs=[pl.BlockSpec(memory_space=pl.ANY)] * 9,
            out_specs=[pl.BlockSpec(memory_space=pl.ANY)] * 9,
            scratch_shapes=[dma((9,))],
            cost_estimate=pl.CostEstimate(flops=30_000_000, bytes_accessed=48_000_000, transcendentals=0),
            compiler_params=pltpu.CompilerParams(vmem_limit_bytes=VMEM),
            name="put_out",
        )(*out)
        swap = [(i, i ^ 1) for i in range(16)]
        own[0], out = lax.optimization_barrier((own[0], out))
        other = [lax.ppermute(own[0], "dp", swap)]
        own, out, other = lax.optimization_barrier((own, out, other))
        other += [lax.ppermute(one, "dp", swap) for one in own[1:]]
        arrived = {(k, whose): (own, other)[whose][k] for k in range(3) for whose in range(2)}
        new = out[:3]
        for items in (((0, 0), (1, 0), (2, 0), (0, 1)), ((1, 1), (2, 1))):
            n = len(items)
            new = pl.pallas_call(
                functools.partial(put_rest, items),
                out_shape=[jax.ShapeDtypeStruct(one.shape, one.dtype) for one in weights],
                in_specs=[pl.BlockSpec(memory_space=pltpu.VMEM)] * n + [pl.BlockSpec(memory_space=pl.ANY)] * 3,
                out_specs=[pl.BlockSpec(memory_space=pl.ANY)] * 3,
                scratch_shapes=[dma((n,))],
                input_output_aliases={n: 0, n + 1: 1, n + 2: 2},
                cost_estimate=pl.CostEstimate(flops=3_000_000, bytes_accessed=5_000_000, transcendentals=0),
                compiler_params=pltpu.CompilerParams(vmem_limit_bytes=VMEM),
                name="put_rest",
            )(*[arrived[item] for item in items], *new)
        out = [*new, *out[3:]]
        return tuple(out)

    all_of, cut = P(None, None, None), P(None, "dp", None)
    step = jax.shard_map(
        step,
        mesh=mesh,
        in_specs=(P(("rep", "dp"), None, None, None),) * 3 + (all_of,) * 3 + (cut,) * 6,
        out_specs=(P("rep", None, None),) * 3 + (P("rep", "dp", None),) * 6,
        check_vma=False,
    )
    return step
```

```python
import functools

import jax
import jax.numpy as jnp
from jax import lax
from jax.experimental import pallas as pl
from jax.experimental.pallas import tpu as pltpu
from jax.sharding import PartitionSpec as P


X, Y, Z = 4, 2, 1
ORDERS = ((X, Y, Z), (Y, Z, X), (Z, X, Y))
LAYERS = 2
HALVES = 2
CHUNKS = tuple((layer, half) for layer in range(LAYERS) for half in range(HALVES))
LAST = len(CHUNKS) - 1
TILE = 16
VMEM = 15 * 512 * 1024
THEIRS, LAND1, LAND2, LAND3, OLD = 0, 8, 12, 14, 15
RING = 12
STAGES = ((0, 4), (4, 2), (6, 1), (7, 1))


def ring():
    order = [(stage, c) for stage in range(4) for c in range(len(CHUNKS))]
    place, then, holder, unit = {}, {}, {}, 0
    for stage, c in order:
        count = STAGES[stage][1]
        place[stage, c] = unit % RING
        blocks = [(unit + i) % RING for i in range(count)]
        before = [holder[b] for b in blocks if b in holder]
        then.setdefault(max(before, key=order.index) if before else None, []).append((stage, c))
        holder.update({b: (stage, c) for b in blocks})
        unit += count
    return place, then


PLACE, THEN = ring()
TURN = {0: (0, 1, 1, 0), 1: (1, 1, 1, 1), 2: (0, 0, 0, 0), 3: (1, 1, 1, 1)}
FIRST = {(0, 0): 4, (0, 1): 8, (0, 3): 4, (1, 0): 8, (2, 0): 4, (3, 0): 4}


def slots(order):
    d1, d2, d3 = order
    kept = [d2 ^ d3, d2, d3, 0]
    return [d1 ^ r for r in kept] + kept


def total(refs):
    acc = refs[0].astype(jnp.float32)
    for one in refs[1:]:
        acc = acc + one.astype(jnp.float32)
    return acc


def kernel(*refs):
    g, w, m, v, out_w, out_m, out_v, later, mine = (refs[i : i + 3] for i in range(0, 27, 3))
    (pair_send, pair_first, pair_recv, pair_kept, mine_sem, rs_send, rs_recv) = refs[27:34]
    (state_sem, free, ag_send, agp_send) = refs[34:]

    me = lax.axis_index("dp")
    core = lax.rem(me, 2)
    bits = {Z: lax.rem(lax.div(me, 2), 2), Y: lax.rem(lax.div(me, 4), 2), X: lax.div(me, 8)}

    def chip(mask):
        return sum(d * ((1 - bits[d]) if mask & d else bits[d]) for d in (X, Y, Z))

    def at(mask):
        return {"dp": chip(mask) * 2 + core}

    partner = {"dp": me + 1 - 2 * core}
    peers = (partner, at(X), at(Y), at(Z))
    rows_of = [one.shape[1] for one in m]

    def rows(k, mask, which, half):
        size = rows_of[k] // HALVES
        start = (chip(mask) * 2 + which) * rows_of[k] + half * size
        return pl.ds(pl.multiple_of(start, TILE), size)

    def part(k, half, slot=0):
        size = rows_of[k] // HALVES
        return pl.ds(slot * rows_of[k] + half * size, size)

    def remote(src, dst, send, recv, device):
        return pltpu.make_async_remote_copy(
            src_ref=src, dst_ref=dst, send_sem=send, recv_sem=recv, device_id=device, device_id_type=pl.DeviceIdType.MESH
        )

    events = [(c, layer, half, k) for c, (layer, half) in enumerate(CHUNKS) for k in range(3)]

    def load_mine(k, after):
        for stage, c in THEN.get(after, []):
            layer, half = CHUNKS[c]
            first, count = STAGES[stage]
            for j, r in enumerate(slots(ORDERS[k])[first : first + count]):
                source = g[k].at[layer, rows(k, r, core, half)]
                pltpu.make_async_copy(source, mine[k].at[PLACE[stage, c] + j], mine_sem.at[TURN[stage][c], k]).start()

    def pair(k, c, layer, half, slot):
        r = slots(ORDERS[k])[slot]
        arrived = pair_kept.at[k] if slot > 3 else pair_recv.at[k, c - 1] if c else pair_first.at[k, slot]
        here = out_w[k].at[layer, part(k, half, THEIRS + slot)]
        return remote(g[k].at[layer, rows(k, r, 1 - core, half)], here, pair_send.at[k], arrived, partner)

    for k in range(3):
        load_mine(k, None)

    barrier = pltpu.get_barrier_semaphore()
    for peer in peers:
        pl.semaphore_signal(barrier, inc=1, device_id=peer, device_id_type=pl.DeviceIdType.MESH)
    pl.semaphore_wait(barrier, 4)

    def pair_chunk(c, group):
        for slot in range(4 * group, 4 * group + 4):
            for k in range(3):
                pair(k, c, *CHUNKS[c], slot).start()

    pair_chunk(0, 0)
    pair_chunk(1, 0)

    def arrival(k, blocks, sem):
        spot = out_w[k].at[0, pl.ds(0, blocks * rows_of[k] // HALVES)]
        return remote(spot, spot, pair_send.at[k], sem, partner)

    def departure(k, blocks, sem):
        spot = out_w[k].at[0, pl.ds(0, blocks * rows_of[k] // HALVES)]
        return remote(spot, spot, sem, pair_kept.at[k], partner)

    def wait_mine(k, c, stage):
        if (stage, c) in FIRST:
            spot = mine[k].at[pl.ds(0, FIRST[stage, c])]
            pltpu.make_async_copy(spot, spot, mine_sem.at[TURN[stage][c], k]).wait()

    def step_of(k):
        return TILE * (1 if k < 2 else 3)

    def slot_rows(k, half, slot, i):
        return pl.ds(pl.multiple_of(slot * rows_of[k] + half * (rows_of[k] // HALVES) + i * step_of(k), TILE), step_of(k))

    def add(k, c, layer, half, stage, begin, count, extra):
        first = STAGES[stage][0] + begin
        steps = rows_of[k] // HALVES // step_of(k)

        def body(n, _):
            j, i = lax.div(n, steps), lax.rem(n, steps)
            here = slot_rows(k, half, THEIRS + first + j, i)
            terms = [out_w[k][layer, here], mine[k][PLACE[stage, c] + begin + j, slot_rows(k, 0, 0, i)]]
            terms += [out_w[k][layer, slot_rows(k, half, slot + j, i)] for slot in extra]
            out_w[k][layer, here] = total(terms).astype(jnp.bfloat16)
            return 0

        lax.fori_loop(0, count * steps, body, 0)

    def hop(stage, k, c, layer, half, begin, count):
        first = STAGES[stage][0]
        land = (LAND1, LAND2, LAND3)[stage]
        for j in range(begin, begin + count):
            source = out_w[k].at[layer, part(k, half, THEIRS + first + j)]
            target = out_w[k].at[layer, part(k, half, land + j)]
            remote(source, target, rs_send.at[k, c], rs_recv.at[stage, k, c], at(ORDERS[k][stage])).start()

    for slot in range(4):
        for k in range(3):
            if slot == 0:
                wait_mine(k, 0, 0)
            arrival(k, 1, pair_first.at[k, slot]).wait_recv()
            add(k, 0, *CHUNKS[0], 0, slot, 1, [])
            hop(0, k, 0, *CHUNKS[0], slot, 1)
    for c, group in ((2, 0), (3, 0), (0, 1), (1, 1), (2, 1), (3, 1)):
        pair_chunk(c, group)
    for k in range(3):
        load_mine(k, (0, 0))
    for c, layer, half, k in events[3:]:
        wait_mine(k, c, 0)
        arrival(k, 4, pair_recv.at[k, c - 1]).wait_recv()
        add(k, c, layer, half, 0, 0, 4, [])
        hop(0, k, c, layer, half, 0, 4)
        load_mine(k, (0, c))

    def state(k, layer, half):
        here = part(k, half)
        return [
            pltpu.make_async_copy(w[k].at[layer, rows(k, 0, core, half)], out_w[k].at[layer, part(k, half, OLD)], state_sem.at[k]),
            pltpu.make_async_copy(m[k].at[layer, here], out_m[k].at[layer, here], state_sem.at[k]),
            pltpu.make_async_copy(v[k].at[layer, here], out_v[k].at[layer, here], state_sem.at[k]),
        ]

    for c, layer, half, k in events:
        for copy in state(k, layer, half):
            copy.start()

    for c, layer, half, k in events:
        if c == 0:
            arrival(k, 4 * len(CHUNKS), pair_kept.at[k]).wait_recv()
        wait_mine(k, c, 1)
        arrival(k, 4, rs_recv.at[0, k, c]).wait_recv()
        add(k, c, layer, half, 1, 0, 2, [LAND1])
        hop(1, k, c, layer, half, 0, 2)
        load_mine(k, (1, c))
    for c, layer, half, k in events:
        wait_mine(k, c, 2)
        arrival(k, 2, rs_recv.at[1, k, c]).wait_recv()
        add(k, c, layer, half, 2, 0, 1, [LAND1 + 2, LAND2])
        hop(2, k, c, layer, half, 0, 1)

    def adamw(k, c, layer, half):
        steps = rows_of[k] // HALVES // step_of(k)

        def body(i, _):
            here = slot_rows(k, half, 0, i)
            terms = [out_w[k][layer, slot_rows(k, half, slot, i)] for slot in (THEIRS + 7, LAND1 + 3, LAND2 + 1, LAND3)]
            terms.append(mine[k][PLACE[3, c], slot_rows(k, 0, 0, i)])
            grad = total(terms).astype(jnp.bfloat16).astype(jnp.float32)
            old = out_w[k][layer, slot_rows(k, half, OLD, i)].astype(jnp.float32)
            new_m = 0.9 * out_m[k][layer, here] + 0.1 * grad
            new_v = 0.95 * out_v[k][layer, here] + 0.05 * grad * grad
            out_m[k][layer, here] = new_m
            out_v[k][layer, here] = new_v
            new = old - 0.02 * (new_m * lax.rsqrt(new_v + 1e-8) + 0.1 * old)
            out_w[k][layer, slot_rows(k, half, me, i)] = new.astype(jnp.bfloat16)
            return 0

        lax.fori_loop(0, steps, body, 0)

    def gathered(k, c, mask):
        d1, d2, d3 = ORDERS[k]
        if not mask & d1:
            return rs_recv.at[(d3, d2, d2 ^ d3).index(mask), k, c]
        return pair_first.at[k, (0, d3, d2, d2 ^ d3).index(mask ^ d1)] if c == LAST - 1 else pair_recv.at[k, c]

    def set_aside(k, layer, half, mask, place):
        start = (chip(mask) * 2 + core) * rows_of[k] + half * (rows_of[k] // HALVES)

        def body(i, _):
            there = pl.ds(pl.multiple_of(start + i * step_of(k), TILE), step_of(k))
            later[k][place, slot_rows(k, 0, 0, i)] = out_w[k][layer, there]
            return 0

        lax.fori_loop(0, rows_of[k] // HALVES // step_of(k), body, 0)

    def gather(k, c, layer, half, mask, dim):
        _, d2, d3 = ORDERS[k]
        d = ORDERS[k][dim]
        spot = out_w[k].at[layer, rows(k, mask, core, half)]
        if dim == 0 and c == LAST:
            set_aside(k, layer, half, mask, (0, d3, d2, d2 ^ d3).index(mask))
        else:
            remote(spot, spot, ag_send.at[k], gathered(k, c, mask ^ d), at(d)).start()

    def wait_gather(k, c, mask):
        arrival(k, 1, gathered(k, c, mask)).wait_recv()

    def to_partner(k, layer, half, mask):
        spot = out_w[k].at[layer, rows(k, mask, core, half)]
        return remote(spot, spot, agp_send.at[k], pair_kept.at[k], partner)

    def send_own(c, layer, half, k):
        pl.semaphore_wait(free.at[k, c], 4)
        for dim in (2, 1, 0):
            gather(k, c, layer, half, 0, dim)
        to_partner(k, layer, half, 0).start()

    for n, (c, layer, half, k) in enumerate(events):
        if c == 0:
            held = out_w[k].at[0, pl.ds(0, 10 * rows_of[k])]
            pltpu.make_async_copy(held, held, state_sem.at[k]).wait()
        wait_mine(k, c, 3)
        arrival(k, 1, rs_recv.at[2, k, c]).wait_recv()
        departure(k, 7, rs_send.at[k, c]).wait_send()
        adamw(k, c, layer, half)
        for peer in peers:
            pl.semaphore_signal(free.at[k, c], inc=1, device_id=peer, device_id_type=pl.DeviceIdType.MESH)
        if n:
            send_own(*events[n - 1])
    send_own(*events[-1])

    for c, layer, half, k in events:
        d1, d2, d3 = ORDERS[k]
        wait_gather(k, c, d3)
        for dim in (1, 0):
            gather(k, c, layer, half, d3, dim)
        to_partner(k, layer, half, d3).start()
    for c, (layer, half) in enumerate(CHUNKS):
        for far in range(2):
            for k, (d1, d2, d3) in enumerate(ORDERS):
                mask = d2 ^ d3 * far
                wait_gather(k, c, mask)
                gather(k, c, layer, half, mask, 0)
                to_partner(k, layer, half, mask).start()
    for c, (layer, half) in enumerate(CHUNKS[:LAST]):
        for which in range(4):
            for k, (d1, d2, d3) in enumerate(ORDERS):
                if c == LAST - 1:
                    arrival(k, 1, pair_first.at[k, which]).wait_recv()
                elif which == 0:
                    arrival(k, 4, pair_recv.at[k, c]).wait_recv()
                to_partner(k, layer, half, d1 ^ (0, d3, d2, d2 ^ d3)[which]).start()

    n = len(CHUNKS)
    for k in range(3):
        departure(k, 8 * n, pair_send.at[k]).wait_send()
        departure(k, 7 * n - 4, ag_send.at[k]).wait_send()
        departure(k, 8 * n - 4, agp_send.at[k]).wait_send()
        arrival(k, 8 * n - 4, pair_kept.at[k]).wait_recv()


def put_out(*refs):
    sources, targets, sem = refs[:9], refs[9:18], refs[18]
    for i, (source, target) in enumerate(zip(sources, targets, strict=True)):
        for layer in range(LAYERS):
            for j in range(4):
                here = pl.ds(j * (source.shape[1] // 4), source.shape[1] // 4)
                pltpu.make_async_copy(source.at[layer, here], target.at[layer, here], sem.at[i]).start()
    for i, (source, target) in enumerate(zip(sources, targets, strict=True)):
        pltpu.make_async_copy(source, target, sem.at[i]).wait()


def put_rest(items, *refs):
    n = len(items)
    sources, out_w, sem = refs[:n], refs[n + 3 : n + 6], refs[n + 6]
    me = lax.axis_index("dp")
    core = lax.rem(me, 2)
    bits = {Z: lax.rem(lax.div(me, 2), 2), Y: lax.rem(lax.div(me, 4), 2), X: lax.div(me, 8)}
    layer, half = CHUNKS[LAST]
    for i, (k, whose) in enumerate(items):
        d1, d2, d3 = ORDERS[k]
        size = sources[i].shape[1]
        for j, r in enumerate((0, d3, d2, d2 ^ d3)):
            chip = sum(d * ((1 - bits[d]) if (d1 ^ r) & d else bits[d]) for d in (X, Y, Z))
            which = 1 - core if whose else core
            start = ((chip * 2 + which) * HALVES + half) * size
            target = out_w[k].at[layer, pl.ds(pl.multiple_of(start, TILE), size)]
            pltpu.make_async_copy(sources[i].at[j], target, sem.at[i]).start()
    for i in range(n):
        pltpu.make_async_copy(sources[i], sources[i], sem.at[i]).wait()


def solution(mesh):
    def step(*arrays):
        terms = [one.reshape(one.shape[1:]) for one in arrays[:3]]
        weights, m, v = arrays[3:6], arrays[6:9], arrays[9:12]
        blocks = [one.shape[1:] for one in m]
        n = len(CHUNKS)

        dma = pltpu.SemaphoreType.DMA
        out = pl.pallas_call(
            kernel,
            out_shape=[pltpu.VMEM(one.shape, one.dtype) for one in (*weights, *m, *v)]
            + [pltpu.VMEM((4, rows // HALVES, columns), jnp.bfloat16) for rows, columns in blocks],
            in_specs=[pl.BlockSpec(memory_space=pl.ANY)] * 12,
            out_specs=[pl.BlockSpec(memory_space=pltpu.VMEM)] * 12,
            scratch_shapes=[
                *[pltpu.VMEM((RING, rows // HALVES, columns), jnp.bfloat16) for rows, columns in blocks],
                dma((3,)),
                dma((3, 4)),
                dma((3, n - 1)),
                dma((3,)),
                dma((2, 3)),
                dma((3, n)),
                dma((3, 3, n)),
                dma((3,)),
                pltpu.SemaphoreType.REGULAR((3, n)),
                dma((3,)),
                dma((3,)),
            ],
            compiler_params=pltpu.CompilerParams(collective_id=0, has_side_effects=True, vmem_limit_bytes=VMEM),
            name="step",
        )(*terms, *weights, *m, *v)
        out, later = out[:9], out[9:]
        own = []
        for k in range(3):
            own.append(lax.ppermute(later[k], "dp", [(i, i ^ 2 * ORDERS[k][0]) for i in range(16)]))
        out = pl.pallas_call(
            put_out,
            out_shape=[jax.ShapeDtypeStruct(one.shape, one.dtype) for one in (*weights, *m, *v)],
            in_specs=[pl.BlockSpec(memory_space=pl.ANY)] * 9,
            out_specs=[pl.BlockSpec(memory_space=pl.ANY)] * 9,
            scratch_shapes=[dma((9,))],
            cost_estimate=pl.CostEstimate(flops=30_000_000, bytes_accessed=48_000_000, transcendentals=0),
            compiler_params=pltpu.CompilerParams(vmem_limit_bytes=VMEM),
            name="put_out",
        )(*out)
        other = []
        for k in range(3):
            other.append(lax.ppermute(own[k], "dp", [(i, i ^ 1) for i in range(16)]))
        arrived = {(k, whose): (own, other)[whose][k] for k in range(3) for whose in range(2)}
        new = out[:3]
        for items in (((0, 0), (1, 0), (2, 0), (0, 1)), ((1, 1), (2, 1))):
            n = len(items)
            new = pl.pallas_call(
                functools.partial(put_rest, items),
                out_shape=[jax.ShapeDtypeStruct(one.shape, one.dtype) for one in weights],
                in_specs=[pl.BlockSpec(memory_space=pltpu.VMEM)] * n + [pl.BlockSpec(memory_space=pl.ANY)] * 3,
                out_specs=[pl.BlockSpec(memory_space=pl.ANY)] * 3,
                scratch_shapes=[dma((n,))],
                input_output_aliases={n: 0, n + 1: 1, n + 2: 2},
                cost_estimate=pl.CostEstimate(flops=3_000_000, bytes_accessed=5_000_000, transcendentals=0),
                compiler_params=pltpu.CompilerParams(vmem_limit_bytes=VMEM),
                name="put_rest",
            )(*[arrived[item] for item in items], *new)
        out = [*new, *out[3:]]
        return tuple(out)

    all_of, cut = P(None, None, None), P(None, "dp", None)
    step = jax.shard_map(
        step,
        mesh=mesh,
        in_specs=(P(("rep", "dp"), None, None, None),) * 3 + (all_of,) * 3 + (cut,) * 6,
        out_specs=(P("rep", None, None),) * 3 + (P("rep", "dp", None),) * 6,
        check_vma=False,
    )
    return step
```

```python
import functools

import jax
import jax.numpy as jnp
from jax import lax
from jax.experimental import pallas as pl
from jax.experimental.pallas import tpu as pltpu
from jax.sharding import PartitionSpec as P


X, Y, Z = 4, 2, 1
ORDERS = ((X, Y, Z), (Y, Z, X), (Z, X, Y))
LAYERS = 2
HALVES = 2
CHUNKS = tuple((layer, half) for layer in range(LAYERS) for half in range(HALVES))
LAST = len(CHUNKS) - 1
TILE = 16
VMEM = 15 * 512 * 1024
THEIRS, LAND1, LAND2, LAND3, OLD = 0, 8, 12, 14, 15
RING = 12
STAGES = ((0, 4), (4, 2), (6, 1), (7, 1))


def ring():
    order = [(stage, c) for stage in range(4) for c in range(len(CHUNKS))]
    place, then, holder, unit = {}, {}, {}, 0
    for stage, c in order:
        count = STAGES[stage][1]
        place[stage, c] = unit % RING
        blocks = [(unit + i) % RING for i in range(count)]
        before = [holder[b] for b in blocks if b in holder]
        then.setdefault(max(before, key=order.index) if before else None, []).append((stage, c))
        holder.update({b: (stage, c) for b in blocks})
        unit += count
    return place, then


PLACE, THEN = ring()
TURN = {0: (0, 1, 1, 0), 1: (1, 1, 1, 1), 2: (0, 0, 0, 0), 3: (1, 1, 1, 1)}
CROSS = ((0, (0, 1, 2, 3)), (1, (0, 1, 2, 3)), (2, (0, 1, 2)), (2, (3,)))
FIRST = {(0, 0): 4, (0, 1): 8, (0, 3): 4, (1, 0): 8, (2, 0): 4, (3, 0): 4}


def slots(order):
    d1, d2, d3 = order
    kept = [d2 ^ d3, d2, d3, 0]
    return [d1 ^ r for r in kept] + kept


def far(order):
    _, d2, d3 = order
    return (0, d3, d2, d2 ^ d3)


def total(refs):
    acc = refs[0].astype(jnp.float32)
    for one in refs[1:]:
        acc = acc + one.astype(jnp.float32)
    return acc


def kernel(*refs):
    g, w, m, v, out_w, out_m, out_v = (refs[i : i + 3] for i in range(0, 21, 3))
    later, hand, mine = refs[21 : 21 + len(CROSS)], refs[21 + len(CROSS) : 24 + len(CROSS)], refs[24 + len(CROSS) : 27 + len(CROSS)]
    (pair_send, pair_first, pair_recv, pair_kept, mine_sem, rs_send, rs_recv) = refs[27 + len(CROSS) : 34 + len(CROSS)]
    (state_sem, free, ag_send, agp_send) = refs[34 + len(CROSS) :]

    me = lax.axis_index("dp")
    core = lax.rem(me, 2)
    bits = {Z: lax.rem(lax.div(me, 2), 2), Y: lax.rem(lax.div(me, 4), 2), X: lax.div(me, 8)}

    def chip(mask):
        return sum(d * ((1 - bits[d]) if mask & d else bits[d]) for d in (X, Y, Z))

    def at(mask):
        return {"dp": chip(mask) * 2 + core}

    partner = {"dp": me + 1 - 2 * core}
    peers = (partner, at(X), at(Y), at(Z))
    rows_of = [one.shape[1] for one in m]

    def rows(k, mask, which, half, piece=None):
        size = rows_of[k] // HALVES
        start = (chip(mask) * 2 + which) * rows_of[k] + half * size
        if piece is not None:
            size = size // 2
            start = start + piece * size
        return pl.ds(pl.multiple_of(start, TILE), size)

    def part(k, half, slot=0, piece=None):
        size = rows_of[k] // HALVES
        if piece is None:
            return pl.ds(slot * rows_of[k] + half * size, size)
        return pl.ds(slot * rows_of[k] + half * size + piece * (size // 2), size // 2)

    def remote(src, dst, send, recv, device):
        return pltpu.make_async_remote_copy(
            src_ref=src, dst_ref=dst, send_sem=send, recv_sem=recv, device_id=device, device_id_type=pl.DeviceIdType.MESH
        )

    events = [(c, layer, half, k) for c, (layer, half) in enumerate(CHUNKS) for k in range(3)]

    def load_mine(k, after):
        for stage, c in THEN.get(after, []):
            layer, half = CHUNKS[c]
            first, count = STAGES[stage]
            for j, r in enumerate(slots(ORDERS[k])[first : first + count]):
                source = g[k].at[layer, rows(k, r, core, half)]
                pltpu.make_async_copy(source, mine[k].at[PLACE[stage, c] + j], mine_sem.at[TURN[stage][c], k]).start()

    def pair(k, c, layer, half, slot, piece=None):
        r = slots(ORDERS[k])[slot]
        arrived = pair_kept.at[k] if slot > 3 else pair_recv.at[k, c - 1] if c else pair_first.at[k, 4 if piece == 0 else slot]
        here = out_w[k].at[layer, part(k, half, THEIRS + slot, piece)]
        return remote(g[k].at[layer, rows(k, r, 1 - core, half, piece)], here, pair_send.at[k], arrived, partner)

    barrier = pltpu.get_barrier_semaphore()
    for peer in peers:
        pl.semaphore_signal(barrier, inc=1, device_id=peer, device_id_type=pl.DeviceIdType.MESH)
    for k in range(3):
        load_mine(k, None)
    pl.semaphore_wait(barrier, 4)

    def pair_chunk(c, group):
        for slot in range(4 * group, 4 * group + 4):
            for piece in (0, 1) if c == slot == 0 else (None,):
                for k in range(3):
                    pair(k, c, *CHUNKS[c], slot, piece).start()

    pair_chunk(0, 0)
    pair_chunk(1, 0)

    def arrival(k, blocks, sem):
        spot = out_w[k].at[0, pl.ds(0, blocks * rows_of[k] // HALVES)]
        return remote(spot, spot, pair_send.at[k], sem, partner)

    def half_arrival(k, sem):
        spot = out_w[k].at[0, pl.ds(0, rows_of[k] // HALVES // 2)]
        return remote(spot, spot, pair_send.at[k], sem, partner)

    def departure(k, blocks, sem):
        spot = out_w[k].at[0, pl.ds(0, blocks * rows_of[k] // HALVES)]
        return remote(spot, spot, sem, pair_kept.at[k], partner)

    def wait_mine(k, c, stage):
        if (stage, c) in FIRST:
            spot = mine[k].at[pl.ds(0, FIRST[stage, c])]
            pltpu.make_async_copy(spot, spot, mine_sem.at[TURN[stage][c], k]).wait()

    def step_of(k):
        return TILE * (1 if k < 2 else 3)

    def slot_rows(k, half, slot, i):
        return pl.ds(pl.multiple_of(slot * rows_of[k] + half * (rows_of[k] // HALVES) + i * step_of(k), TILE), step_of(k))

    def add(k, c, layer, half, stage, begin, count, extra, piece=None):
        first = STAGES[stage][0] + begin
        steps = rows_of[k] // HALVES // step_of(k)
        low, high = (0, count * steps) if piece is None else (piece * steps // 2, (piece + 1) * steps // 2)

        def body(n, _):
            j, i = lax.div(n, steps), lax.rem(n, steps)
            here = slot_rows(k, half, THEIRS + first + j, i)
            terms = [out_w[k][layer, here], mine[k][PLACE[stage, c] + begin + j, slot_rows(k, 0, 0, i)]]
            terms += [out_w[k][layer, slot_rows(k, half, slot + j, i)] for slot in extra]
            out_w[k][layer, here] = total(terms).astype(jnp.bfloat16)
            return 0

        lax.fori_loop(low, high, body, 0)

    def hop(stage, k, c, layer, half, begin, count, piece=None):
        first = STAGES[stage][0]
        land = (LAND1, LAND2, LAND3)[stage]
        for j in range(begin, begin + count):
            source = out_w[k].at[layer, part(k, half, THEIRS + first + j, piece)]
            target = out_w[k].at[layer, part(k, half, land + j, piece)]
            remote(source, target, rs_send.at[k, c], rs_recv.at[stage, k, c], at(ORDERS[k][stage])).start()

    for slot, piece in ((0, 0), (0, 1), (1, None), (2, None), (3, None)):
        for k in range(3):
            if piece == 0:
                wait_mine(k, 0, 0)
            if slot == 0:
                half_arrival(k, pair_first.at[k, 4 * (1 - piece)]).wait_recv()
            else:
                arrival(k, 1, pair_first.at[k, slot]).wait_recv()
            add(k, 0, *CHUNKS[0], 0, slot, 1, [], piece)
            hop(0, k, 0, *CHUNKS[0], slot, 1, piece)
    for c, group in ((2, 0), (3, 0), (0, 1), (1, 1), (2, 1), (3, 1)):
        pair_chunk(c, group)
    for k in range(3):
        load_mine(k, (0, 0))
    for c, layer, half, k in events[3:]:
        wait_mine(k, c, 0)
        arrival(k, 4, pair_recv.at[k, c - 1]).wait_recv()
        add(k, c, layer, half, 0, 0, 4, [])
        hop(0, k, c, layer, half, 0, 4)
        load_mine(k, (0, c))

    def state(k, layer, half):
        here = part(k, half)
        return [
            pltpu.make_async_copy(w[k].at[layer, rows(k, 0, core, half)], out_w[k].at[layer, part(k, half, OLD)], state_sem.at[k]),
            pltpu.make_async_copy(m[k].at[layer, here], out_m[k].at[layer, here], state_sem.at[k]),
            pltpu.make_async_copy(v[k].at[layer, here], out_v[k].at[layer, here], state_sem.at[k]),
        ]

    for c, layer, half, k in events:
        for copy in state(k, layer, half):
            copy.start()

    for c, layer, half, k in events:
        if c == 0:
            arrival(k, 4 * len(CHUNKS), pair_kept.at[k]).wait_recv()
        wait_mine(k, c, 1)
        arrival(k, 4, rs_recv.at[0, k, c]).wait_recv()
        add(k, c, layer, half, 1, 0, 2, [LAND1])
        hop(1, k, c, layer, half, 0, 2)
        load_mine(k, (1, c))
    for c, layer, half, k in events:
        wait_mine(k, c, 2)
        arrival(k, 2, rs_recv.at[1, k, c]).wait_recv()
        add(k, c, layer, half, 2, 0, 1, [LAND1 + 2, LAND2])
        hop(2, k, c, layer, half, 0, 1)

    def adamw(k, c, layer, half):
        steps = rows_of[k] // HALVES // step_of(k)

        def body(i, _):
            here = slot_rows(k, half, 0, i)
            terms = [out_w[k][layer, slot_rows(k, half, slot, i)] for slot in (THEIRS + 7, LAND1 + 3, LAND2 + 1, LAND3)]
            terms.append(mine[k][PLACE[3, c], slot_rows(k, 0, 0, i)])
            grad = total(terms).astype(jnp.bfloat16).astype(jnp.float32)
            old = out_w[k][layer, slot_rows(k, half, OLD, i)].astype(jnp.float32)
            new_m = 0.9 * out_m[k][layer, here] + 0.1 * grad
            new_v = 0.95 * out_v[k][layer, here] + 0.05 * grad * grad
            out_m[k][layer, here] = new_m
            out_v[k][layer, here] = new_v
            new = old - 0.02 * (new_m * lax.rsqrt(new_v + 1e-8) + 0.1 * old)
            out_w[k][layer, slot_rows(k, half, me, i)] = new.astype(jnp.bfloat16)
            return 0

        lax.fori_loop(0, steps, body, 0)

    def gathered(k, c, mask):
        d1, d2, d3 = ORDERS[k]
        if not mask & d1:
            return rs_recv.at[(d3, d2, d2 ^ d3).index(mask), k, c]
        return pair_first.at[k, (0, d3, d2, d2 ^ d3).index(mask ^ d1)] if c == LAST - 1 else pair_recv.at[k, c]

    def set_aside(k, layer, half, mask, target):
        start = (chip(mask) * 2 + core) * rows_of[k] + half * (rows_of[k] // HALVES)

        def body(i, _):
            there = pl.ds(pl.multiple_of(start + i * step_of(k), TILE), step_of(k))
            target[slot_rows(k, 0, 0, i)] = out_w[k][layer, there]
            return 0

        lax.fori_loop(0, rows_of[k] // HALVES // step_of(k), body, 0)

    def gather(k, c, layer, half, mask, dim):
        d = ORDERS[k][dim]
        spot = out_w[k].at[layer, rows(k, mask, core, half)]
        if dim == 0 and c == LAST:
            place = far(ORDERS[k]).index(mask)
            (target,) = [later[i].at[places.index(place)] for i, (which, places) in enumerate(CROSS) if which == k and place in places]
            set_aside(k, layer, half, mask, target)
        else:
            remote(spot, spot, ag_send.at[k], gathered(k, c, mask ^ d), at(d)).start()

    def wait_gather(k, c, mask):
        arrival(k, 1, gathered(k, c, mask)).wait_recv()

    def to_partner(k, layer, half, mask):
        spot = out_w[k].at[layer, rows(k, mask, core, half)]
        return remote(spot, spot, agp_send.at[k], pair_kept.at[k], partner)

    def send_own(c, layer, half, k):
        pl.semaphore_wait(free.at[k, c], 4)
        for dim in (2, 1, 0):
            gather(k, c, layer, half, 0, dim)
        to_partner(k, layer, half, 0).start()

    for n, (c, layer, half, k) in enumerate(events):
        if c == 0:
            held = out_w[k].at[0, pl.ds(0, 10 * rows_of[k])]
            pltpu.make_async_copy(held, held, state_sem.at[k]).wait()
        wait_mine(k, c, 3)
        arrival(k, 1, rs_recv.at[2, k, c]).wait_recv()
        departure(k, 7, rs_send.at[k, c]).wait_send()
        adamw(k, c, layer, half)
        for peer in peers:
            pl.semaphore_signal(free.at[k, c], inc=1, device_id=peer, device_id_type=pl.DeviceIdType.MESH)
        if n:
            send_own(*events[n - 1])
    send_own(*events[-1])

    for c, layer, half, k in events:
        d1, d2, d3 = ORDERS[k]
        wait_gather(k, c, d3)
        for dim in (1, 0):
            gather(k, c, layer, half, d3, dim)
        to_partner(k, layer, half, d3).start()
    for c, (layer, half) in enumerate(CHUNKS):
        for both in range(2):
            for k, (d1, d2, d3) in enumerate(ORDERS):
                mask = d2 ^ d3 * both
                wait_gather(k, c, mask)
                gather(k, c, layer, half, mask, 0)
                to_partner(k, layer, half, mask).start()
    for c, (layer, half) in enumerate(CHUNKS[:LAST]):
        for which in range(4):
            for k, order in enumerate(ORDERS):
                mask = order[0] ^ far(order)[which]
                if c == LAST - 1:
                    arrival(k, 1, pair_first.at[k, which]).wait_recv()
                elif which == 0:
                    arrival(k, 4, pair_recv.at[k, c]).wait_recv()
                if c == LAST - 1 and which == 3:
                    set_aside(k, layer, half, mask, hand[k])
                else:
                    to_partner(k, layer, half, mask).start()

    n = len(CHUNKS)
    for k in range(3):
        departure(k, 8 * n, pair_send.at[k]).wait_send()
        departure(k, 7 * n - 4, ag_send.at[k]).wait_send()
        departure(k, 8 * n - 5, agp_send.at[k]).wait_send()
        arrival(k, 8 * n - 5, pair_kept.at[k]).wait_recv()


def place_of(mask, size):
    me = lax.axis_index("dp")
    bits = {Z: lax.rem(lax.div(me, 2), 2), Y: lax.rem(lax.div(me, 4), 2), X: lax.div(me, 8)}
    return sum(d * ((1 - bits[d]) if mask & d else bits[d]) for d in (X, Y, Z)) * 2 * size


def put_out(*refs):
    sources, targets, sem = refs[:9], refs[9:18], refs[18]

    def put(i, layer, start, size, which):
        here = pl.ds(start, size)
        pltpu.make_async_copy(sources[i].at[layer, here], targets[i].at[layer, here], sem.at[which]).start()

    layer, half = CHUNKS[LAST]
    for k, (d1, d2, d3) in enumerate(ORDERS):
        size = sources[k].shape[1] // 16
        for j in range(4):
            put(k, 1 - layer, j * 4 * size, 4 * size, k)
        for r in (0, d3, d2, d2 ^ d3):
            put(k, layer, pl.multiple_of(place_of(r, size), TILE), 2 * size, 9 + k)
            for core in range(2):
                start = place_of(d1 ^ r, size) + core * size + (1 - half) * (size // HALVES)
                put(k, layer, pl.multiple_of(start, TILE), size // HALVES, 9 + k)
    for i in range(3, 9):
        for j in range(LAYERS):
            put(i, j, 0, sources[i].shape[1], i)
    for k in range(3):
        size = sources[k].shape[1] // 16
        for which, there in ((k, sources[k].at[0]), (9 + k, sources[k].at[0, pl.ds(0, 12 * size)])):
            pltpu.make_async_copy(there, there, sem.at[which]).wait()
    for i in range(3, 9):
        pltpu.make_async_copy(sources[i], sources[i], sem.at[i]).wait()


def put_rest(items, *refs):
    n = len(items)
    sources, out_w, sem = refs[:n], refs[n + 3 : n + 6], refs[n + 6]
    core = lax.rem(lax.axis_index("dp"), 2)
    for i, (k, c, masks, whose) in enumerate(items):
        layer, half = CHUNKS[c]
        size = sources[i].shape[-2]
        for j, mask in enumerate(masks):
            start = place_of(mask, HALVES * size) + ((1 - core if whose else core) * HALVES + half) * size
            target = out_w[k].at[layer, pl.ds(pl.multiple_of(start, TILE), size)]
            pltpu.make_async_copy(sources[i].at[j], target, sem.at[i]).start()
    for i in range(n):
        pltpu.make_async_copy(sources[i], sources[i], sem.at[i]).wait()


def solution(mesh):
    def step(*arrays):
        terms = [one.reshape(one.shape[1:]) for one in arrays[:3]]
        weights, m, v = arrays[3:6], arrays[6:9], arrays[9:12]
        blocks = [one.shape[1:] for one in m]
        n = len(CHUNKS)

        dma = pltpu.SemaphoreType.DMA
        out = pl.pallas_call(
            kernel,
            out_shape=[pltpu.VMEM(one.shape, one.dtype) for one in (*weights, *m, *v)]
            + [pltpu.VMEM((len(places), blocks[k][0] // HALVES, blocks[k][1]), jnp.bfloat16) for k, places in CROSS]
            + [pltpu.VMEM((rows // HALVES, columns), jnp.bfloat16) for rows, columns in blocks],
            in_specs=[pl.BlockSpec(memory_space=pl.ANY)] * 12,
            out_specs=[pl.BlockSpec(memory_space=pltpu.VMEM)] * (12 + len(CROSS)),
            scratch_shapes=[
                *[pltpu.VMEM((RING, rows // HALVES, columns), jnp.bfloat16) for rows, columns in blocks],
                dma((3,)),
                dma((3, 5)),
                dma((3, n - 1)),
                dma((3,)),
                dma((2, 3)),
                dma((3, n)),
                dma((3, 3, n)),
                dma((3,)),
                pltpu.SemaphoreType.REGULAR((3, n)),
                dma((3,)),
                dma((3,)),
            ],
            compiler_params=pltpu.CompilerParams(collective_id=0, has_side_effects=True, vmem_limit_bytes=VMEM),
            name="step",
        )(*terms, *weights, *m, *v)
        out, later, hand = out[:9], out[9:-3], out[-3:]
        swap = [(i, i ^ 1) for i in range(16)]
        own = []
        for i, (k, _) in enumerate(CROSS):
            own.append(lax.ppermute(later[i], "dp", [(i, i ^ 2 * ORDERS[k][0]) for i in range(16)]))
        handed = []
        for k in range(3):
            handed.append(lax.ppermute(hand[k], "dp", swap)[None])
        out = pl.pallas_call(
            put_out,
            out_shape=[jax.ShapeDtypeStruct(one.shape, one.dtype) for one in (*weights, *m, *v)],
            in_specs=[pl.BlockSpec(memory_space=pl.ANY)] * 9,
            out_specs=[pl.BlockSpec(memory_space=pl.ANY)] * 9,
            scratch_shapes=[dma((12,))],
            cost_estimate=pl.CostEstimate(flops=30_000_000, bytes_accessed=48_000_000, transcendentals=0),
            compiler_params=pltpu.CompilerParams(vmem_limit_bytes=VMEM),
            name="put_out",
        )(*out)
        other = []
        for i in range(len(CROSS)):
            other.append(lax.ppermute(own[i], "dp", swap))
        arrived = {}
        for i, (k, places) in enumerate(CROSS):
            masks = tuple(ORDERS[k][0] ^ far(ORDERS[k])[place] for place in places)
            arrived[k, LAST, masks, 0], arrived[k, LAST, masks, 1] = own[i], other[i]
        for k, order in enumerate(ORDERS):
            arrived[k, LAST - 1, (order[0] ^ far(order)[3],), 1] = handed[k]
        final = [item for item, block in arrived.items() if any(block is one for one in (other[0], other[1], other[3]))]
        new = out[:3]
        for items in ([item for item in arrived if item not in final], final):
            n = len(items)
            new = pl.pallas_call(
                functools.partial(put_rest, items),
                out_shape=[jax.ShapeDtypeStruct(one.shape, one.dtype) for one in weights],
                in_specs=[pl.BlockSpec(memory_space=pltpu.VMEM)] * n + [pl.BlockSpec(memory_space=pl.ANY)] * 3,
                out_specs=[pl.BlockSpec(memory_space=pl.ANY)] * 3,
                scratch_shapes=[dma((n,))],
                input_output_aliases={n: 0, n + 1: 1, n + 2: 2},
                cost_estimate=pl.CostEstimate(flops=3_000_000, bytes_accessed=5_000_000, transcendentals=0),
                compiler_params=pltpu.CompilerParams(vmem_limit_bytes=VMEM),
                name="put_rest",
            )(*[arrived[item] for item in items], *new)
        out = [*new, *out[3:]]
        return tuple(out)

    all_of, cut = P(None, None, None), P(None, "dp", None)
    step = jax.shard_map(
        step,
        mesh=mesh,
        in_specs=(P(("rep", "dp"), None, None, None),) * 3 + (all_of,) * 3 + (cut,) * 6,
        out_specs=(P("rep", None, None),) * 3 + (P("rep", "dp", None),) * 6,
        check_vma=False,
    )
    return step
```

```python
import functools

import jax
import jax.numpy as jnp
from jax import lax
from jax.experimental import pallas as pl
from jax.experimental.pallas import tpu as pltpu
from jax.sharding import PartitionSpec as P


X, Y, Z = 4, 2, 1
ORDERS = ((X, Y, Z), (Y, Z, X), (Z, X, Y))
LAYERS = 2
HALVES = 2
CHUNKS = tuple((layer, half) for layer in range(LAYERS) for half in range(HALVES))
LAST = len(CHUNKS) - 1
TILE = 16
VMEM = 15 * 512 * 1024
THEIRS, LAND1, LAND2, LAND3, OLD = 0, 8, 12, 14, 15
RING = 12
STAGES = ((0, 4), (4, 2), (6, 1), (7, 1))


def ring():
    order = [(stage, c) for stage in range(4) for c in range(len(CHUNKS))]
    place, then, holder, unit = {}, {}, {}, 0
    for stage, c in order:
        count = STAGES[stage][1]
        place[stage, c] = unit % RING
        blocks = [(unit + i) % RING for i in range(count)]
        before = [holder[b] for b in blocks if b in holder]
        then.setdefault(max(before, key=order.index) if before else None, []).append((stage, c))
        holder.update({b: (stage, c) for b in blocks})
        unit += count
    return place, then


PLACE, THEN = ring()
TURN = {0: (0, 1, 1, 0), 1: (1, 1, 1, 1), 2: (0, 0, 0, 0), 3: (1, 1, 1, 1)}
CROSS = ((0, (0, 1, 2, 3)), (1, (0, 1, 2, 3)), (2, (0, 1, 2)), (2, (3,)))
FIRST = {(0, 0): 4, (0, 1): 8, (0, 3): 4, (1, 0): 8, (2, 0): 4, (3, 0): 4}


def slots(order):
    d1, d2, d3 = order
    kept = [d2 ^ d3, d2, d3, 0]
    return [d1 ^ r for r in kept] + kept


def far(order):
    _, d2, d3 = order
    return (0, d3, d2, d2 ^ d3)


def total(refs):
    acc = refs[0].astype(jnp.float32)
    for one in refs[1:]:
        acc = acc + one.astype(jnp.float32)
    return acc


def kernel(*refs):
    g, w, m, v, out_w, out_m, out_v = (refs[i : i + 3] for i in range(0, 21, 3))
    later, hand, mine = refs[21 : 21 + len(CROSS)], refs[21 + len(CROSS) : 24 + len(CROSS)], refs[24 + len(CROSS) : 27 + len(CROSS)]
    (pair_send, pair_first, pair_recv, pair_kept, mine_sem, rs_send, rs_recv) = refs[27 + len(CROSS) : 34 + len(CROSS)]
    (state_sem, free, ag_send, agp_send) = refs[34 + len(CROSS) :]

    me = lax.axis_index("dp")
    core = lax.rem(me, 2)
    bits = {Z: lax.rem(lax.div(me, 2), 2), Y: lax.rem(lax.div(me, 4), 2), X: lax.div(me, 8)}

    def chip(mask):
        return sum(d * ((1 - bits[d]) if mask & d else bits[d]) for d in (X, Y, Z))

    def at(mask):
        return {"dp": chip(mask) * 2 + core}

    partner = {"dp": me + 1 - 2 * core}
    peers = (partner, at(X), at(Y), at(Z))
    rows_of = [one.shape[1] for one in m]

    def rows(k, mask, which, half, piece=None):
        size = rows_of[k] // HALVES
        start = (chip(mask) * 2 + which) * rows_of[k] + half * size
        if piece is not None:
            size = size // 2
            start = start + piece * size
        return pl.ds(pl.multiple_of(start, TILE), size)

    def part(k, half, slot=0, piece=None):
        size = rows_of[k] // HALVES
        if piece is None:
            return pl.ds(slot * rows_of[k] + half * size, size)
        return pl.ds(slot * rows_of[k] + half * size + piece * (size // 2), size // 2)

    def remote(src, dst, send, recv, device):
        return pltpu.make_async_remote_copy(
            src_ref=src, dst_ref=dst, send_sem=send, recv_sem=recv, device_id=device, device_id_type=pl.DeviceIdType.MESH
        )

    events = [(c, layer, half, k) for c, (layer, half) in enumerate(CHUNKS) for k in range(3)]

    def load_mine(k, after):
        for stage, c in THEN.get(after, []):
            layer, half = CHUNKS[c]
            first, count = STAGES[stage]
            for j, r in enumerate(slots(ORDERS[k])[first : first + count]):
                source = g[k].at[layer, rows(k, r, core, half)]
                pltpu.make_async_copy(source, mine[k].at[PLACE[stage, c] + j], mine_sem.at[TURN[stage][c], k]).start()

    def pair(k, c, layer, half, slot, piece=None):
        r = slots(ORDERS[k])[slot]
        arrived = pair_kept.at[k] if slot > 3 else pair_recv.at[k, c // 2] if c else pair_first.at[k, 4 if piece == 0 else slot]
        here = out_w[k].at[layer, part(k, half, THEIRS + slot, piece)]
        return remote(g[k].at[layer, rows(k, r, 1 - core, half, piece)], here, pair_send.at[k], arrived, partner)

    barrier = pltpu.get_barrier_semaphore()
    for peer in peers:
        pl.semaphore_signal(barrier, inc=1, device_id=peer, device_id_type=pl.DeviceIdType.MESH)
    for k in range(3):
        load_mine(k, None)
    pl.semaphore_wait(barrier, 4)

    def pair_chunk(c, group):
        for slot in range(4 * group, 4 * group + 4):
            for piece in (0, 1) if c == slot == 0 else (None,):
                for k in range(3):
                    pair(k, c, *CHUNKS[c], slot, piece).start()

    pair_chunk(0, 0)
    pair_chunk(1, 0)

    def arrival(k, blocks, sem):
        spot = out_w[k].at[0, pl.ds(0, blocks * rows_of[k] // HALVES)]
        return remote(spot, spot, pair_send.at[k], sem, partner)

    def half_arrival(k, sem):
        spot = out_w[k].at[0, pl.ds(0, rows_of[k] // HALVES // 2)]
        return remote(spot, spot, pair_send.at[k], sem, partner)

    def departure(k, blocks, sem):
        spot = out_w[k].at[0, pl.ds(0, blocks * rows_of[k] // HALVES)]
        return remote(spot, spot, sem, pair_kept.at[k], partner)

    def wait_mine(k, c, stage):
        if (stage, c) in FIRST:
            spot = mine[k].at[pl.ds(0, FIRST[stage, c])]
            pltpu.make_async_copy(spot, spot, mine_sem.at[TURN[stage][c], k]).wait()

    def step_of(k):
        return TILE * (1 if k < 2 else 3)

    def slot_rows(k, half, slot, i):
        return pl.ds(pl.multiple_of(slot * rows_of[k] + half * (rows_of[k] // HALVES) + i * step_of(k), TILE), step_of(k))

    def add(k, c, layer, half, stage, begin, count, extra, piece=None):
        first = STAGES[stage][0] + begin
        steps = rows_of[k] // HALVES // step_of(k)
        low, high = (0, count * steps) if piece is None else (piece * steps // 2, (piece + 1) * steps // 2)

        def body(n, _):
            j, i = lax.div(n, steps), lax.rem(n, steps)
            here = slot_rows(k, half, THEIRS + first + j, i)
            terms = [out_w[k][layer, here], mine[k][PLACE[stage, c] + begin + j, slot_rows(k, 0, 0, i)]]
            terms += [out_w[k][layer, slot_rows(k, half, slot + j, i)] for slot in extra]
            out_w[k][layer, here] = total(terms).astype(jnp.bfloat16)
            return 0

        lax.fori_loop(low, high, body, 0)

    def hop(stage, k, c, layer, half, begin, count, piece=None):
        first = STAGES[stage][0]
        land = (LAND1, LAND2, LAND3)[stage]
        for j in range(begin, begin + count):
            source = out_w[k].at[layer, part(k, half, THEIRS + first + j, piece)]
            target = out_w[k].at[layer, part(k, half, land + j, piece)]
            remote(source, target, rs_send.at[k, c // 2], rs_recv.at[stage, k, c // 2], at(ORDERS[k][stage])).start()

    for slot, piece in ((0, 0), (0, 1), (1, None), (2, None), (3, None)):
        for k in range(3):
            if piece == 0:
                wait_mine(k, 0, 0)
            if slot == 0:
                half_arrival(k, pair_first.at[k, 4 * (1 - piece)]).wait_recv()
            else:
                arrival(k, 1, pair_first.at[k, slot]).wait_recv()
            add(k, 0, *CHUNKS[0], 0, slot, 1, [], piece)
            hop(0, k, 0, *CHUNKS[0], slot, 1, piece)
    for c, group in ((2, 0), (3, 0), (0, 1), (1, 1), (2, 1), (3, 1)):
        pair_chunk(c, group)
    for k in range(3):
        load_mine(k, (0, 0))
    for c, layer, half, k in events[3:]:
        wait_mine(k, c, 0)
        if c < 3:
            arrival(k, 4 * c, pair_recv.at[k, c // 2]).wait_recv()
        add(k, c, layer, half, 0, 0, 4, [])
        hop(0, k, c, layer, half, 0, 4)
        load_mine(k, (0, c))

    def state(k, layer, half):
        here = part(k, half)
        return [
            pltpu.make_async_copy(w[k].at[layer, rows(k, 0, core, half)], out_w[k].at[layer, part(k, half, OLD)], state_sem.at[k]),
            pltpu.make_async_copy(m[k].at[layer, here], out_m[k].at[layer, here], state_sem.at[k]),
            pltpu.make_async_copy(v[k].at[layer, here], out_v[k].at[layer, here], state_sem.at[k]),
        ]

    for c, layer, half, k in events:
        for copy in state(k, layer, half):
            copy.start()

    for c, layer, half, k in events:
        if c == 0:
            arrival(k, 4 * len(CHUNKS), pair_kept.at[k]).wait_recv()
        wait_mine(k, c, 1)
        if c % 2 == 0:
            arrival(k, 8, rs_recv.at[0, k, c // 2]).wait_recv()
        add(k, c, layer, half, 1, 0, 2, [LAND1])
        hop(1, k, c, layer, half, 0, 2)
        load_mine(k, (1, c))
    for c, layer, half, k in events:
        wait_mine(k, c, 2)
        if c % 2 == 0:
            arrival(k, 4, rs_recv.at[1, k, c // 2]).wait_recv()
        add(k, c, layer, half, 2, 0, 1, [LAND1 + 2, LAND2])
        hop(2, k, c, layer, half, 0, 1)

    def adamw(k, c, layer, half):
        steps = rows_of[k] // HALVES // step_of(k)

        def body(i, _):
            here = slot_rows(k, half, 0, i)
            terms = [out_w[k][layer, slot_rows(k, half, slot, i)] for slot in (THEIRS + 7, LAND1 + 3, LAND2 + 1, LAND3)]
            terms.append(mine[k][PLACE[3, c], slot_rows(k, 0, 0, i)])
            grad = total(terms).astype(jnp.bfloat16).astype(jnp.float32)
            old = out_w[k][layer, slot_rows(k, half, OLD, i)].astype(jnp.float32)
            new_m = 0.9 * out_m[k][layer, here] + 0.1 * grad
            new_v = 0.95 * out_v[k][layer, here] + 0.05 * grad * grad
            out_m[k][layer, here] = new_m
            out_v[k][layer, here] = new_v
            new = old - 0.02 * (new_m * lax.rsqrt(new_v + 1e-8) + 0.1 * old)
            out_w[k][layer, slot_rows(k, half, me, i)] = new.astype(jnp.bfloat16)
            return 0

        lax.fori_loop(0, steps, body, 0)

    def gathered(k, c, mask):
        d1, d2, d3 = ORDERS[k]
        if not mask & d1:
            return rs_recv.at[(d3, d2, d2 ^ d3).index(mask), k, c // 2]
        return pair_first.at[k, (0, d3, d2, d2 ^ d3).index(mask ^ d1)] if c == LAST - 1 else pair_recv.at[k, c]

    def set_aside(k, layer, half, mask, target):
        start = (chip(mask) * 2 + core) * rows_of[k] + half * (rows_of[k] // HALVES)

        def body(i, _):
            there = pl.ds(pl.multiple_of(start + i * step_of(k), TILE), step_of(k))
            target[slot_rows(k, 0, 0, i)] = out_w[k][layer, there]
            return 0

        lax.fori_loop(0, rows_of[k] // HALVES // step_of(k), body, 0)

    def gather(k, c, layer, half, mask, dim):
        d = ORDERS[k][dim]
        spot = out_w[k].at[layer, rows(k, mask, core, half)]
        if dim == 0 and c == LAST:
            place = far(ORDERS[k]).index(mask)
            (target,) = [later[i].at[places.index(place)] for i, (which, places) in enumerate(CROSS) if which == k and place in places]
            set_aside(k, layer, half, mask, target)
        else:
            remote(spot, spot, ag_send.at[k], gathered(k, c, mask ^ d), at(d)).start()

    def wait_gather(k, c, mask):
        if c % 2 == 0:
            arrival(k, 2, gathered(k, c, mask)).wait_recv()

    def to_partner(k, layer, half, mask):
        spot = out_w[k].at[layer, rows(k, mask, core, half)]
        return remote(spot, spot, agp_send.at[k], pair_kept.at[k], partner)

    for first in range(0, len(CHUNKS), 2):
        two = [event for event in events if event[0] // 2 == first // 2]
        for c, layer, half, k in two:
            if c == 0:
                held = out_w[k].at[0, pl.ds(0, 10 * rows_of[k])]
                pltpu.make_async_copy(held, held, state_sem.at[k]).wait()
            wait_mine(k, c, 3)
            if c == first:
                arrival(k, 2, rs_recv.at[2, k, first // 2]).wait_recv()
                departure(k, 14, rs_send.at[k, first // 2]).wait_send()
            adamw(k, c, layer, half)
            if c > first:
                for peer in peers:
                    pl.semaphore_signal(free.at[k, first // 2], inc=1, device_id=peer, device_id_type=pl.DeviceIdType.MESH)
        for c, layer, half, k in two:
            if c == first:
                pl.semaphore_wait(free.at[k, first // 2], 4)
            for dim in (2, 1, 0):
                gather(k, c, layer, half, 0, dim)
            to_partner(k, layer, half, 0).start()

    for c, layer, half, k in events:
        d1, d2, d3 = ORDERS[k]
        wait_gather(k, c, d3)
        for dim in (1, 0):
            gather(k, c, layer, half, d3, dim)
        to_partner(k, layer, half, d3).start()
    for c, (layer, half) in enumerate(CHUNKS):
        for both in range(2):
            for k, (d1, d2, d3) in enumerate(ORDERS):
                mask = d2 ^ d3 * both
                wait_gather(k, c, mask)
                gather(k, c, layer, half, mask, 0)
                to_partner(k, layer, half, mask).start()
    for c, (layer, half) in enumerate(CHUNKS[:LAST]):
        for which in range(4):
            for k, order in enumerate(ORDERS):
                mask = order[0] ^ far(order)[which]
                if c == LAST - 1:
                    arrival(k, 1, pair_first.at[k, which]).wait_recv()
                elif which == 0:
                    arrival(k, 4, pair_recv.at[k, c]).wait_recv()
                if c == LAST - 1 and which == 3:
                    set_aside(k, layer, half, mask, hand[k])
                else:
                    to_partner(k, layer, half, mask).start()

    n = len(CHUNKS)
    for k in range(3):
        departure(k, 8 * n, pair_send.at[k]).wait_send()
        departure(k, 7 * n - 4, ag_send.at[k]).wait_send()
        departure(k, 8 * n - 5, agp_send.at[k]).wait_send()
        arrival(k, 8 * n - 5, pair_kept.at[k]).wait_recv()


def place_of(mask, size):
    me = lax.axis_index("dp")
    bits = {Z: lax.rem(lax.div(me, 2), 2), Y: lax.rem(lax.div(me, 4), 2), X: lax.div(me, 8)}
    return sum(d * ((1 - bits[d]) if mask & d else bits[d]) for d in (X, Y, Z)) * 2 * size


def put_out(*refs):
    sources, targets, sem = refs[:9], refs[9:18], refs[18]

    def put(i, layer, start, size, which):
        here = pl.ds(start, size)
        pltpu.make_async_copy(sources[i].at[layer, here], targets[i].at[layer, here], sem.at[which]).start()

    layer, half = CHUNKS[LAST]
    for k, (d1, d2, d3) in enumerate(ORDERS):
        size = sources[k].shape[1] // 16
        for j in range(4):
            put(k, 1 - layer, j * 4 * size, 4 * size, k)
        for r in (0, d3, d2, d2 ^ d3):
            put(k, layer, pl.multiple_of(place_of(r, size), TILE), 2 * size, 9 + k)
            for core in range(2):
                start = place_of(d1 ^ r, size) + core * size + (1 - half) * (size // HALVES)
                put(k, layer, pl.multiple_of(start, TILE), size // HALVES, 9 + k)
    for i in range(3, 9):
        for j in range(LAYERS):
            put(i, j, 0, sources[i].shape[1], i)
    for k in range(3):
        size = sources[k].shape[1] // 16
        for which, there in ((k, sources[k].at[0]), (9 + k, sources[k].at[0, pl.ds(0, 12 * size)])):
            pltpu.make_async_copy(there, there, sem.at[which]).wait()
    for i in range(3, 9):
        pltpu.make_async_copy(sources[i], sources[i], sem.at[i]).wait()


def put_rest(items, *refs):
    n = len(items)
    sources, out_w, sem = refs[:n], refs[n + 3 : n + 6], refs[n + 6]
    core = lax.rem(lax.axis_index("dp"), 2)
    for i, (k, c, masks, whose) in enumerate(items):
        layer, half = CHUNKS[c]
        size = sources[i].shape[-2]
        for j, mask in enumerate(masks):
            start = place_of(mask, HALVES * size) + ((1 - core if whose else core) * HALVES + half) * size
            target = out_w[k].at[layer, pl.ds(pl.multiple_of(start, TILE), size)]
            pltpu.make_async_copy(sources[i].at[j], target, sem.at[i]).start()
    for i in range(n):
        pltpu.make_async_copy(sources[i], sources[i], sem.at[i]).wait()


def solution(mesh):
    def step(*arrays):
        terms = [one.reshape(one.shape[1:]) for one in arrays[:3]]
        weights, m, v = arrays[3:6], arrays[6:9], arrays[9:12]
        blocks = [one.shape[1:] for one in m]
        n = len(CHUNKS)

        dma = pltpu.SemaphoreType.DMA
        out = pl.pallas_call(
            kernel,
            out_shape=[pltpu.VMEM(one.shape, one.dtype) for one in (*weights, *m, *v)]
            + [pltpu.VMEM((len(places), blocks[k][0] // HALVES, blocks[k][1]), jnp.bfloat16) for k, places in CROSS]
            + [pltpu.VMEM((rows // HALVES, columns), jnp.bfloat16) for rows, columns in blocks],
            in_specs=[pl.BlockSpec(memory_space=pl.ANY)] * 12,
            out_specs=[pl.BlockSpec(memory_space=pltpu.VMEM)] * (12 + len(CROSS)),
            scratch_shapes=[
                *[pltpu.VMEM((RING, rows // HALVES, columns), jnp.bfloat16) for rows, columns in blocks],
                dma((3,)),
                dma((3, 5)),
                dma((3, 2)),
                dma((3,)),
                dma((2, 3)),
                dma((3, n // 2)),
                dma((3, 3, n // 2)),
                dma((3,)),
                pltpu.SemaphoreType.REGULAR((3, n // 2)),
                dma((3,)),
                dma((3,)),
            ],
            compiler_params=pltpu.CompilerParams(collective_id=0, has_side_effects=True, vmem_limit_bytes=VMEM),
            name="step",
        )(*terms, *weights, *m, *v)
        out, later, hand = out[:9], out[9:-3], out[-3:]
        swap = [(i, i ^ 1) for i in range(16)]
        own = []
        for i, (k, _) in enumerate(CROSS):
            own.append(lax.ppermute(later[i], "dp", [(i, i ^ 2 * ORDERS[k][0]) for i in range(16)]))
        handed = []
        for k in range(3):
            handed.append(lax.ppermute(hand[k], "dp", swap)[None])
        out = pl.pallas_call(
            put_out,
            out_shape=[jax.ShapeDtypeStruct(one.shape, one.dtype) for one in (*weights, *m, *v)],
            in_specs=[pl.BlockSpec(memory_space=pl.ANY)] * 9,
            out_specs=[pl.BlockSpec(memory_space=pl.ANY)] * 9,
            scratch_shapes=[dma((12,))],
            cost_estimate=pl.CostEstimate(flops=30_000_000, bytes_accessed=48_000_000, transcendentals=0),
            compiler_params=pltpu.CompilerParams(vmem_limit_bytes=VMEM),
            name="put_out",
        )(*out)
        other = []
        for i in range(len(CROSS)):
            other.append(lax.ppermute(own[i], "dp", swap))
        arrived = {}
        for i, (k, places) in enumerate(CROSS):
            masks = tuple(ORDERS[k][0] ^ far(ORDERS[k])[place] for place in places)
            arrived[k, LAST, masks, 0], arrived[k, LAST, masks, 1] = own[i], other[i]
        for k, order in enumerate(ORDERS):
            arrived[k, LAST - 1, (order[0] ^ far(order)[3],), 1] = handed[k]
        calls = ((own[0], own[2], *handed), (own[1], own[3], other[0], other[2]), (other[1], other[3]))
        rest = [[item for item, block in arrived.items() if any(block is one for one in call)] for call in calls]
        new = out[:3]
        for items in rest:
            n = len(items)
            new = pl.pallas_call(
                functools.partial(put_rest, items),
                out_shape=[jax.ShapeDtypeStruct(one.shape, one.dtype) for one in weights],
                in_specs=[pl.BlockSpec(memory_space=pltpu.VMEM)] * n + [pl.BlockSpec(memory_space=pl.ANY)] * 3,
                out_specs=[pl.BlockSpec(memory_space=pl.ANY)] * 3,
                scratch_shapes=[dma((n,))],
                input_output_aliases={n: 0, n + 1: 1, n + 2: 2},
                cost_estimate=pl.CostEstimate(flops=3_000_000, bytes_accessed=5_000_000, transcendentals=0),
                compiler_params=pltpu.CompilerParams(vmem_limit_bytes=VMEM),
                name="put_rest",
            )(*[arrived[item] for item in items], *new)
        out = [*new, *out[3:]]
        return tuple(out)

    all_of, cut = P(None, None, None), P(None, "dp", None)
    step = jax.shard_map(
        step,
        mesh=mesh,
        in_specs=(P(("rep", "dp"), None, None, None),) * 3 + (all_of,) * 3 + (cut,) * 6,
        out_specs=(P("rep", None, None),) * 3 + (P("rep", "dp", None),) * 6,
        check_vma=False,
    )
    return step
```

```python
import functools

import jax
import jax.numpy as jnp
from jax import lax
from jax.experimental import pallas as pl
from jax.experimental.pallas import tpu as pltpu
from jax.sharding import PartitionSpec as P


X, Y, Z = 4, 2, 1
ORDERS = ((X, Y, Z), (Y, Z, X), (Z, X, Y))
LAYERS = 2
HALVES = 2
CHUNKS = tuple((layer, half) for layer in range(LAYERS) for half in range(HALVES))
LAST = len(CHUNKS) - 1
TILE = 16
VMEM = 15 * 512 * 1024
THEIRS, LAND1, LAND2, LAND3, OLD = 0, 8, 12, 14, 15
RING = 12
STAGES = ((0, 4), (4, 2), (6, 1), (7, 1))


def ring():
    order = [(stage, c) for stage in range(4) for c in range(len(CHUNKS))]
    place, then, holder, unit = {}, {}, {}, 0
    for stage, c in order:
        count = STAGES[stage][1]
        place[stage, c] = unit % RING
        blocks = [(unit + i) % RING for i in range(count)]
        before = [holder[b] for b in blocks if b in holder]
        then.setdefault(max(before, key=order.index) if before else None, []).append((stage, c))
        holder.update({b: (stage, c) for b in blocks})
        unit += count
    return place, then


PLACE, THEN = ring()
TURN = {0: (0, 1, 1, 0), 1: (1, 1, 1, 1), 2: (0, 0, 0, 0), 3: (1, 1, 1, 1)}
CROSS = ((0, (0, 1, 2, 3)), (1, (0, 1, 2, 3)), (2, (0, 1, 2)), (2, (3,)))
FIRST = {(0, 0): 4, (0, 1): 8, (0, 3): 4, (1, 0): 8, (2, 0): 4, (3, 0): 4}


def slots(order):
    d1, d2, d3 = order
    kept = [d2 ^ d3, d2, d3, 0]
    return [d1 ^ r for r in kept] + kept


def far(order):
    _, d2, d3 = order
    return (0, d3, d2, d2 ^ d3)


def total(refs):
    acc = refs[0].astype(jnp.float32)
    for one in refs[1:]:
        acc = acc + one.astype(jnp.float32)
    return acc


def kernel(*refs):
    g, w, m, v, out_w, out_m, out_v = (refs[i : i + 3] for i in range(0, 21, 3))
    later, hand, mine = refs[21 : 21 + len(CROSS)], refs[21 + len(CROSS) : 24 + len(CROSS)], refs[24 + len(CROSS) : 27 + len(CROSS)]
    (pair_send, pair_first, pair_recv, pair_kept, mine_sem, rs_recv, free, agp_send) = refs[27 + len(CROSS) :]
    state_sem = ag_send = pair_send

    me = lax.axis_index("dp")
    core = lax.rem(me, 2)
    bits = {Z: lax.rem(lax.div(me, 2), 2), Y: lax.rem(lax.div(me, 4), 2), X: lax.div(me, 8)}

    def chip(mask):
        return sum(d * ((1 - bits[d]) if mask & d else bits[d]) for d in (X, Y, Z))

    def at(mask):
        return {"dp": chip(mask) * 2 + core}

    partner = {"dp": me + 1 - 2 * core}
    peers = (partner, at(X), at(Y), at(Z))
    rows_of = [one.shape[1] for one in m]

    def rows(k, mask, which, half, piece=None):
        size = rows_of[k] // HALVES
        start = (chip(mask) * 2 + which) * rows_of[k] + half * size
        if piece is not None:
            size = size // 2
            start = start + piece * size
        return pl.ds(pl.multiple_of(start, TILE), size)

    def part(k, half, slot=0, piece=None):
        size = rows_of[k] // HALVES
        if piece is None:
            return pl.ds(slot * rows_of[k] + half * size, size)
        return pl.ds(slot * rows_of[k] + half * size + piece * (size // 2), size // 2)

    def remote(src, dst, send, recv, device):
        return pltpu.make_async_remote_copy(
            src_ref=src, dst_ref=dst, send_sem=send, recv_sem=recv, device_id=device, device_id_type=pl.DeviceIdType.MESH
        )

    events = [(c, layer, half, k) for c, (layer, half) in enumerate(CHUNKS) for k in range(3)]

    def load_mine(k, after):
        for stage, c in THEN.get(after, []):
            layer, half = CHUNKS[c]
            first, count = STAGES[stage]
            for j, r in enumerate(slots(ORDERS[k])[first : first + count]):
                source = g[k].at[layer, rows(k, r, core, half)]
                pltpu.make_async_copy(source, mine[k].at[PLACE[stage, c] + j], mine_sem.at[TURN[stage][c], k]).start()

    def pair(k, c, layer, half, slot, piece=None):
        r = slots(ORDERS[k])[slot]
        arrived = pair_kept.at[k] if slot > 3 else pair_recv.at[k, c // 2] if c else pair_first.at[k, 4 if piece == 0 else slot]
        here = out_w[k].at[layer, part(k, half, THEIRS + slot, piece)]
        return remote(g[k].at[layer, rows(k, r, 1 - core, half, piece)], here, pair_send.at[k], arrived, partner)

    barrier = pltpu.get_barrier_semaphore()
    for peer in peers:
        pl.semaphore_signal(barrier, inc=1, device_id=peer, device_id_type=pl.DeviceIdType.MESH)
    for k in range(3):
        load_mine(k, None)
    pl.semaphore_wait(barrier, 4)

    def pair_chunk(c, group):
        for slot in range(4 * group, 4 * group + 4):
            for piece in (0, 1) if c == slot == 0 else (None,):
                for k in range(3):
                    pair(k, c, *CHUNKS[c], slot, piece).start()

    pair_chunk(0, 0)
    pair_chunk(1, 0)

    def arrival(k, blocks, sem):
        spot = out_w[k].at[0, pl.ds(0, blocks * rows_of[k] // HALVES)]
        return remote(spot, spot, pair_send.at[k], sem, partner)

    def half_arrival(k, sem):
        spot = out_w[k].at[0, pl.ds(0, rows_of[k] // HALVES // 2)]
        return remote(spot, spot, pair_send.at[k], sem, partner)

    def departure(k, blocks, sem):
        spot = out_w[k].at[0, pl.ds(0, blocks * rows_of[k] // HALVES)]
        return remote(spot, spot, sem, pair_kept.at[k], partner)

    def wait_mine(k, c, stage):
        if (stage, c) in FIRST:
            spot = mine[k].at[pl.ds(0, FIRST[stage, c])]
            pltpu.make_async_copy(spot, spot, mine_sem.at[TURN[stage][c], k]).wait()

    def step_of(k):
        return TILE * (1 if k < 2 else 3)

    def slot_rows(k, half, slot, i):
        return pl.ds(pl.multiple_of(slot * rows_of[k] + half * (rows_of[k] // HALVES) + i * step_of(k), TILE), step_of(k))

    def add(k, c, layer, half, stage, begin, count, extra, piece=None):
        first = STAGES[stage][0] + begin
        steps = rows_of[k] // HALVES // step_of(k)
        low, high = (0, count * steps) if piece is None else (piece * steps // 2, (piece + 1) * steps // 2)

        def body(n, _):
            j, i = lax.div(n, steps), lax.rem(n, steps)
            here = slot_rows(k, half, THEIRS + first + j, i)
            terms = [out_w[k][layer, here], mine[k][PLACE[stage, c] + begin + j, slot_rows(k, 0, 0, i)]]
            terms += [out_w[k][layer, slot_rows(k, half, slot + j, i)] for slot in extra]
            out_w[k][layer, here] = total(terms).astype(jnp.bfloat16)
            return 0

        lax.fori_loop(low, high, body, 0)

    def rs_sent(k, c):
        return pair_first.at[k, 0 if c // 2 else 4]

    def hop(stage, k, c, layer, half, begin, count, piece=None):
        first = STAGES[stage][0]
        land = (LAND1, LAND2, LAND3)[stage]
        for j in range(begin, begin + count):
            source = out_w[k].at[layer, part(k, half, THEIRS + first + j, piece)]
            target = out_w[k].at[layer, part(k, half, land + j, piece)]
            remote(source, target, rs_sent(k, c), rs_recv.at[stage, k, c // 2], at(ORDERS[k][stage])).start()

    for slot, piece in ((0, 0), (0, 1), (1, None), (2, None), (3, None)):
        for k in range(3):
            if piece == 0:
                wait_mine(k, 0, 0)
            if slot == 0:
                half_arrival(k, pair_first.at[k, 4 * (1 - piece)]).wait_recv()
            else:
                arrival(k, 1, pair_first.at[k, slot]).wait_recv()
            add(k, 0, *CHUNKS[0], 0, slot, 1, [], piece)
            hop(0, k, 0, *CHUNKS[0], slot, 1, piece)
    for c, group in ((2, 0), (3, 0), (0, 1), (1, 1), (2, 1), (3, 1)):
        pair_chunk(c, group)
    for k in range(3):
        load_mine(k, (0, 0))
    for c, layer, half, k in events[3:]:
        wait_mine(k, c, 0)
        if c < 3:
            arrival(k, 4 * c, pair_recv.at[k, c // 2]).wait_recv()
        add(k, c, layer, half, 0, 0, 4, [])
        hop(0, k, c, layer, half, 0, 4)
        load_mine(k, (0, c))

    def state(k, layer, half):
        here = part(k, half)
        return [
            pltpu.make_async_copy(w[k].at[layer, rows(k, 0, core, half)], out_w[k].at[layer, part(k, half, OLD)], state_sem.at[k]),
            pltpu.make_async_copy(m[k].at[layer, here], out_m[k].at[layer, here], state_sem.at[k]),
            pltpu.make_async_copy(v[k].at[layer, here], out_v[k].at[layer, here], state_sem.at[k]),
        ]

    for c, layer, half, k in events:
        if c == 0:
            arrival(k, 4 * len(CHUNKS), pair_kept.at[k]).wait_recv()
            departure(k, 8 * len(CHUNKS), pair_send.at[k]).wait_send()
            for place in CHUNKS:
                for copy in state(k, *place):
                    copy.start()
        wait_mine(k, c, 1)
        if c % 2 == 0:
            arrival(k, 8, rs_recv.at[0, k, c // 2]).wait_recv()
        add(k, c, layer, half, 1, 0, 2, [LAND1])
        hop(1, k, c, layer, half, 0, 2)
        load_mine(k, (1, c))
    for c, layer, half, k in events:
        wait_mine(k, c, 2)
        if c % 2 == 0:
            arrival(k, 4, rs_recv.at[1, k, c // 2]).wait_recv()
        add(k, c, layer, half, 2, 0, 1, [LAND1 + 2, LAND2])
        hop(2, k, c, layer, half, 0, 1)

    def adamw(k, c, layer, half):
        steps = rows_of[k] // HALVES // step_of(k)

        def body(i, _):
            here = slot_rows(k, half, 0, i)
            terms = [out_w[k][layer, slot_rows(k, half, slot, i)] for slot in (THEIRS + 7, LAND1 + 3, LAND2 + 1, LAND3)]
            terms.append(mine[k][PLACE[3, c], slot_rows(k, 0, 0, i)])
            grad = total(terms).astype(jnp.bfloat16).astype(jnp.float32)
            old = out_w[k][layer, slot_rows(k, half, OLD, i)].astype(jnp.float32)
            new_m = 0.9 * out_m[k][layer, here] + 0.1 * grad
            new_v = 0.95 * out_v[k][layer, here] + 0.05 * grad * grad
            out_m[k][layer, here] = new_m
            out_v[k][layer, here] = new_v
            new = old - 0.02 * (new_m * lax.rsqrt(new_v + 1e-8) + 0.1 * old)
            out_w[k][layer, slot_rows(k, half, me, i)] = new.astype(jnp.bfloat16)
            return 0

        lax.fori_loop(0, steps, body, 0)

    def gathered(k, c, mask):
        d1, d2, d3 = ORDERS[k]
        if not mask & d1:
            return rs_recv.at[(d3, d2, d2 ^ d3).index(mask), k, c // 2]
        return pair_first.at[k, (0, d3, d2, d2 ^ d3).index(mask ^ d1)] if c == LAST - 1 else pair_recv.at[k, c]

    def set_aside(k, layer, half, mask, target):
        start = (chip(mask) * 2 + core) * rows_of[k] + half * (rows_of[k] // HALVES)

        def body(i, _):
            there = pl.ds(pl.multiple_of(start + i * step_of(k), TILE), step_of(k))
            target[slot_rows(k, 0, 0, i)] = out_w[k][layer, there]
            return 0

        lax.fori_loop(0, rows_of[k] // HALVES // step_of(k), body, 0)

    def gather(k, c, layer, half, mask, dim):
        d = ORDERS[k][dim]
        spot = out_w[k].at[layer, rows(k, mask, core, half)]
        if dim == 0 and c == LAST:
            place = far(ORDERS[k]).index(mask)
            (target,) = [later[i].at[places.index(place)] for i, (which, places) in enumerate(CROSS) if which == k and place in places]
            set_aside(k, layer, half, mask, target)
        else:
            remote(spot, spot, ag_send.at[k], gathered(k, c, mask ^ d), at(d)).start()

    def wait_gather(k, c, mask):
        if c % 2 == 0:
            arrival(k, 2, gathered(k, c, mask)).wait_recv()

    def to_partner(k, layer, half, mask):
        spot = out_w[k].at[layer, rows(k, mask, core, half)]
        return remote(spot, spot, agp_send.at[k], pair_kept.at[k], partner)

    for first in range(0, len(CHUNKS), 2):
        two = [event for event in events if event[0] // 2 == first // 2]
        for c, layer, half, k in two:
            if c == 0:
                held = out_w[k].at[0, pl.ds(0, 10 * rows_of[k])]
                pltpu.make_async_copy(held, held, state_sem.at[k]).wait()
            wait_mine(k, c, 3)
            if c == first:
                arrival(k, 2, rs_recv.at[2, k, first // 2]).wait_recv()
                departure(k, 14, rs_sent(k, first)).wait_send()
            adamw(k, c, layer, half)
            if c > first:
                for peer in peers:
                    pl.semaphore_signal(free.at[k, first // 2], inc=1, device_id=peer, device_id_type=pl.DeviceIdType.MESH)
        for c, layer, half, k in two:
            if c == first:
                pl.semaphore_wait(free.at[k, first // 2], 4)
            for dim in (2, 1, 0):
                gather(k, c, layer, half, 0, dim)
            to_partner(k, layer, half, 0).start()

    for c, layer, half, k in events:
        d1, d2, d3 = ORDERS[k]
        wait_gather(k, c, d3)
        for dim in (1, 0):
            gather(k, c, layer, half, d3, dim)
        to_partner(k, layer, half, d3).start()
    for c, (layer, half) in enumerate(CHUNKS):
        for both in range(2):
            for k, (d1, d2, d3) in enumerate(ORDERS):
                mask = d2 ^ d3 * both
                wait_gather(k, c, mask)
                gather(k, c, layer, half, mask, 0)
                to_partner(k, layer, half, mask).start()
    for c, (layer, half) in enumerate(CHUNKS[:LAST]):
        for which in range(4):
            for k, order in enumerate(ORDERS):
                mask = order[0] ^ far(order)[which]
                if c == LAST - 1:
                    arrival(k, 1, pair_first.at[k, which]).wait_recv()
                elif which == 0:
                    arrival(k, 4, pair_recv.at[k, c]).wait_recv()
                if c == LAST - 1 and which == 3:
                    set_aside(k, layer, half, mask, hand[k])
                else:
                    to_partner(k, layer, half, mask).start()

    n = len(CHUNKS)
    for k in range(3):
        departure(k, 7 * n - 4, ag_send.at[k]).wait_send()
        departure(k, 8 * n - 5, agp_send.at[k]).wait_send()
        arrival(k, 8 * n - 5, pair_kept.at[k]).wait_recv()


def place_of(mask, size):
    me = lax.axis_index("dp")
    bits = {Z: lax.rem(lax.div(me, 2), 2), Y: lax.rem(lax.div(me, 4), 2), X: lax.div(me, 8)}
    return sum(d * ((1 - bits[d]) if mask & d else bits[d]) for d in (X, Y, Z)) * 2 * size


def put_out(*refs):
    sources, targets, sem = refs[:9], refs[9:18], refs[18]

    def put(i, layer, start, size, which):
        here = pl.ds(start, size)
        pltpu.make_async_copy(sources[i].at[layer, here], targets[i].at[layer, here], sem.at[which]).start()

    layer, half = CHUNKS[LAST]
    for k, (d1, d2, d3) in enumerate(ORDERS):
        size = sources[k].shape[1] // 16
        for j in range(4):
            put(k, 1 - layer, j * 4 * size, 4 * size, k)
        for r in (0, d3, d2, d2 ^ d3):
            put(k, layer, pl.multiple_of(place_of(r, size), TILE), 2 * size, 9 + k)
            for core in range(2):
                start = place_of(d1 ^ r, size) + core * size + (1 - half) * (size // HALVES)
                put(k, layer, pl.multiple_of(start, TILE), size // HALVES, 9 + k)
    for i in range(3, 9):
        for j in range(LAYERS):
            put(i, j, 0, sources[i].shape[1], i)
    for k in range(3):
        size = sources[k].shape[1] // 16
        for which, there in ((k, sources[k].at[0]), (9 + k, sources[k].at[0, pl.ds(0, 12 * size)])):
            pltpu.make_async_copy(there, there, sem.at[which]).wait()
    for i in range(3, 9):
        pltpu.make_async_copy(sources[i], sources[i], sem.at[i]).wait()


def put_rest(items, *refs):
    n = len(items)
    sources, out_w, sem = refs[:n], refs[n + 3 : n + 6], refs[n + 6]
    core = lax.rem(lax.axis_index("dp"), 2)
    for i, (k, c, masks, whose) in enumerate(items):
        layer, half = CHUNKS[c]
        size = sources[i].shape[-2]
        for j, mask in enumerate(masks):
            start = place_of(mask, HALVES * size) + ((1 - core if whose else core) * HALVES + half) * size
            target = out_w[k].at[layer, pl.ds(pl.multiple_of(start, TILE), size)]
            pltpu.make_async_copy(sources[i].at[j], target, sem.at[i]).start()
    for i in range(n):
        pltpu.make_async_copy(sources[i], sources[i], sem.at[i]).wait()


def solution(mesh):
    def step(*arrays):
        terms = [one.reshape(one.shape[1:]) for one in arrays[:3]]
        weights, m, v = arrays[3:6], arrays[6:9], arrays[9:12]
        blocks = [one.shape[1:] for one in m]
        n = len(CHUNKS)

        dma = pltpu.SemaphoreType.DMA
        out = pl.pallas_call(
            kernel,
            out_shape=[pltpu.VMEM(one.shape, one.dtype) for one in (*weights, *m, *v)]
            + [pltpu.VMEM((len(places), blocks[k][0] // HALVES, blocks[k][1]), jnp.bfloat16) for k, places in CROSS]
            + [pltpu.VMEM((rows // HALVES, columns), jnp.bfloat16) for rows, columns in blocks],
            in_specs=[pl.BlockSpec(memory_space=pl.ANY)] * 12,
            out_specs=[pl.BlockSpec(memory_space=pltpu.VMEM)] * (12 + len(CROSS)),
            scratch_shapes=[
                *[pltpu.VMEM((RING, rows // HALVES, columns), jnp.bfloat16) for rows, columns in blocks],
                dma((3,)),
                dma((3, 5)),
                dma((3, 2)),
                dma((3,)),
                dma((2, 3)),
                dma((3, 3, n // 2)),
                pltpu.SemaphoreType.REGULAR((3, n // 2)),
                dma((3,)),
            ],
            compiler_params=pltpu.CompilerParams(collective_id=0, has_side_effects=True, vmem_limit_bytes=VMEM),
            name="step",
        )(*terms, *weights, *m, *v)
        out, later, hand = out[:9], out[9:-3], out[-3:]
        swap = [(i, i ^ 1) for i in range(16)]
        own = []
        for i, (k, _) in enumerate(CROSS):
            own.append(lax.ppermute(later[i], "dp", [(i, i ^ 2 * ORDERS[k][0]) for i in range(16)]))
        handed = []
        for k in range(3):
            handed.append(lax.ppermute(hand[k], "dp", swap)[None])
        out = pl.pallas_call(
            put_out,
            out_shape=[jax.ShapeDtypeStruct(one.shape, one.dtype) for one in (*weights, *m, *v)],
            in_specs=[pl.BlockSpec(memory_space=pl.ANY)] * 9,
            out_specs=[pl.BlockSpec(memory_space=pl.ANY)] * 9,
            scratch_shapes=[dma((12,))],
            cost_estimate=pl.CostEstimate(flops=30_000_000, bytes_accessed=48_000_000, transcendentals=0),
            compiler_params=pltpu.CompilerParams(vmem_limit_bytes=VMEM),
            name="put_out",
        )(*out)
        other = []
        for i in range(len(CROSS)):
            other.append(lax.ppermute(own[i], "dp", swap))
        arrived = {}
        for i, (k, places) in enumerate(CROSS):
            masks = tuple(ORDERS[k][0] ^ far(ORDERS[k])[place] for place in places)
            arrived[k, LAST, masks, 0], arrived[k, LAST, masks, 1] = own[i], other[i]
        for k, order in enumerate(ORDERS):
            arrived[k, LAST - 1, (order[0] ^ far(order)[3],), 1] = handed[k]
        calls = ((own[0], own[2], *handed), (own[1], own[3], other[0], other[2]), (other[1], other[3]))
        rest = [[item for item, block in arrived.items() if any(block is one for one in call)] for call in calls]
        new = out[:3]
        for items in rest:
            n = len(items)
            new = pl.pallas_call(
                functools.partial(put_rest, items),
                out_shape=[jax.ShapeDtypeStruct(one.shape, one.dtype) for one in weights],
                in_specs=[pl.BlockSpec(memory_space=pltpu.VMEM)] * n + [pl.BlockSpec(memory_space=pl.ANY)] * 3,
                out_specs=[pl.BlockSpec(memory_space=pl.ANY)] * 3,
                scratch_shapes=[dma((n,))],
                input_output_aliases={n: 0, n + 1: 1, n + 2: 2},
                cost_estimate=pl.CostEstimate(flops=3_000_000, bytes_accessed=5_000_000, transcendentals=0),
                compiler_params=pltpu.CompilerParams(vmem_limit_bytes=VMEM),
                name="put_rest",
            )(*[arrived[item] for item in items], *new)
        out = [*new, *out[3:]]
        return tuple(out)

    all_of, cut = P(None, None, None), P(None, "dp", None)
    step = jax.shard_map(
        step,
        mesh=mesh,
        in_specs=(P(("rep", "dp"), None, None, None),) * 3 + (all_of,) * 3 + (cut,) * 6,
        out_specs=(P("rep", None, None),) * 3 + (P("rep", "dp", None),) * 6,
        check_vma=False,
    )
    return step
```

```python
import functools

import jax
import jax.numpy as jnp
from jax import lax
from jax.experimental import pallas as pl
from jax.experimental.pallas import tpu as pltpu
from jax.sharding import PartitionSpec as P


X, Y, Z = 4, 2, 1
ORDERS = ((X, Y, Z), (Y, Z, X), (Z, X, Y))
LAYERS = 2
HALVES = 2
CHUNKS = tuple((layer, half) for layer in range(LAYERS) for half in range(HALVES))
LAST = len(CHUNKS) - 1
TILE = 16
VMEM = 15 * 512 * 1024
THEIRS, LAND1, LAND2, LAND3, OLD = 0, 8, 12, 14, 15
RING = 12
STAGES = ((0, 4), (4, 2), (6, 1), (7, 1))


def ring():
    order = [(stage, c) for stage in range(4) for c in range(len(CHUNKS))]
    place, then, holder, unit = {}, {}, {}, 0
    for stage, c in order:
        count = STAGES[stage][1]
        place[stage, c] = unit % RING
        blocks = [(unit + i) % RING for i in range(count)]
        before = [holder[b] for b in blocks if b in holder]
        then.setdefault(max(before, key=order.index) if before else None, []).append((stage, c))
        holder.update({b: (stage, c) for b in blocks})
        unit += count
    return place, then


PLACE, THEN = ring()
TURN = {0: (0, 1, 1, 0), 1: (1, 1, 1, 1), 2: (0, 0, 0, 0), 3: (1, 1, 1, 1)}
CROSS = ((0, (0, 1, 2, 3)), (1, (0, 1, 2, 3)), (2, (0, 1, 2)), (2, (3,)))
FIRST = {(0, 0): 4, (0, 1): 8, (0, 3): 4, (1, 0): 8, (2, 0): 4, (3, 0): 4}


def slots(order):
    d1, d2, d3 = order
    kept = [d2 ^ d3, d2, d3, 0]
    return [d1 ^ r for r in kept] + kept


def far(order):
    _, d2, d3 = order
    return (0, d3, d2, d2 ^ d3)


def total(refs):
    acc = refs[0].astype(jnp.float32)
    for one in refs[1:]:
        acc = acc + one.astype(jnp.float32)
    return acc


def kernel(*refs):
    g, w, m, v, out_w, out_m, out_v = (refs[i : i + 3] for i in range(0, 21, 3))
    later, hand, mine = refs[21 : 21 + len(CROSS)], refs[21 + len(CROSS) : 24 + len(CROSS)], refs[24 + len(CROSS) : 27 + len(CROSS)]
    (pair_send, pair_first, pair_recv, pair_kept, mine_sem, rs_recv, free) = refs[27 + len(CROSS) :]
    state_sem = ag_send = pair_send
    agp_send = mine_sem.at[0]

    me = lax.axis_index("dp")
    core = lax.rem(me, 2)
    bits = {Z: lax.rem(lax.div(me, 2), 2), Y: lax.rem(lax.div(me, 4), 2), X: lax.div(me, 8)}

    def chip(mask):
        return sum(d * ((1 - bits[d]) if mask & d else bits[d]) for d in (X, Y, Z))

    def at(mask):
        return {"dp": chip(mask) * 2 + core}

    partner = {"dp": me + 1 - 2 * core}
    peers = (partner, at(X), at(Y), at(Z))
    rows_of = [one.shape[1] for one in m]

    def rows(k, mask, which, half, piece=None):
        size = rows_of[k] // HALVES
        start = (chip(mask) * 2 + which) * rows_of[k] + half * size
        if piece is not None:
            size = size // 2
            start = start + piece * size
        return pl.ds(pl.multiple_of(start, TILE), size)

    def part(k, half, slot=0, piece=None):
        size = rows_of[k] // HALVES
        if piece is None:
            return pl.ds(slot * rows_of[k] + half * size, size)
        return pl.ds(slot * rows_of[k] + half * size + piece * (size // 2), size // 2)

    def remote(src, dst, send, recv, device):
        return pltpu.make_async_remote_copy(
            src_ref=src, dst_ref=dst, send_sem=send, recv_sem=recv, device_id=device, device_id_type=pl.DeviceIdType.MESH
        )

    events = [(c, layer, half, k) for c, (layer, half) in enumerate(CHUNKS) for k in range(3)]

    def load_mine(k, after):
        for stage, c in THEN.get(after, []):
            layer, half = CHUNKS[c]
            first, count = STAGES[stage]
            for j, r in enumerate(slots(ORDERS[k])[first : first + count]):
                source = g[k].at[layer, rows(k, r, core, half)]
                pltpu.make_async_copy(source, mine[k].at[PLACE[stage, c] + j], mine_sem.at[TURN[stage][c], k]).start()

    def pair(k, c, layer, half, slot, piece=None):
        r = slots(ORDERS[k])[slot]
        arrived = pair_kept.at[k] if slot > 3 else pair_recv.at[k, c // 2] if c else pair_first.at[k, 4 if piece == 0 else slot]
        here = out_w[k].at[layer, part(k, half, THEIRS + slot, piece)]
        return remote(g[k].at[layer, rows(k, r, 1 - core, half, piece)], here, pair_send.at[k], arrived, partner)

    barrier = pltpu.get_barrier_semaphore()
    for peer in peers:
        pl.semaphore_signal(barrier, inc=1, device_id=peer, device_id_type=pl.DeviceIdType.MESH)
    for k in range(3):
        load_mine(k, None)
    pl.semaphore_wait(barrier, 4)

    def pair_chunk(c, group):
        for slot in range(4 * group, 4 * group + 4):
            for piece in (0, 1) if c == slot == 0 else (None,):
                for k in range(3):
                    pair(k, c, *CHUNKS[c], slot, piece).start()

    pair_chunk(0, 0)
    pair_chunk(1, 0)

    def arrival(k, blocks, sem):
        spot = out_w[k].at[0, pl.ds(0, blocks * rows_of[k] // HALVES)]
        return remote(spot, spot, pair_send.at[k], sem, partner)

    def half_arrival(k, sem):
        spot = out_w[k].at[0, pl.ds(0, rows_of[k] // HALVES // 2)]
        return remote(spot, spot, pair_send.at[k], sem, partner)

    def departure(k, blocks, sem):
        spot = out_w[k].at[0, pl.ds(0, blocks * rows_of[k] // HALVES)]
        return remote(spot, spot, sem, pair_kept.at[k], partner)

    def wait_mine(k, c, stage):
        if (stage, c) in FIRST:
            spot = mine[k].at[pl.ds(0, FIRST[stage, c])]
            pltpu.make_async_copy(spot, spot, mine_sem.at[TURN[stage][c], k]).wait()

    def step_of(k):
        return TILE * (1 if k < 2 else 3)

    def slot_rows(k, half, slot, i):
        return pl.ds(pl.multiple_of(slot * rows_of[k] + half * (rows_of[k] // HALVES) + i * step_of(k), TILE), step_of(k))

    def add(k, c, layer, half, stage, begin, count, extra, piece=None):
        first = STAGES[stage][0] + begin
        steps = rows_of[k] // HALVES // step_of(k)
        low, high = (0, count * steps) if piece is None else (piece * steps // 2, (piece + 1) * steps // 2)

        def body(n, _):
            j, i = lax.div(n, steps), lax.rem(n, steps)
            here = slot_rows(k, half, THEIRS + first + j, i)
            terms = [out_w[k][layer, here], mine[k][PLACE[stage, c] + begin + j, slot_rows(k, 0, 0, i)]]
            terms += [out_w[k][layer, slot_rows(k, half, slot + j, i)] for slot in extra]
            out_w[k][layer, here] = total(terms).astype(jnp.bfloat16)
            return 0

        lax.fori_loop(low, high, body, 0)

    def rs_sent(k, c):
        return pair_first.at[k, 0 if c // 2 else 4]

    def hop(stage, k, c, layer, half, begin, count, piece=None):
        first = STAGES[stage][0]
        land = (LAND1, LAND2, LAND3)[stage]
        for j in range(begin, begin + count):
            source = out_w[k].at[layer, part(k, half, THEIRS + first + j, piece)]
            target = out_w[k].at[layer, part(k, half, land + j, piece)]
            remote(source, target, rs_sent(k, c), rs_recv.at[stage, k, c // 2], at(ORDERS[k][stage])).start()

    for slot, piece in ((0, 0), (0, 1), (1, None), (2, None), (3, None)):
        for k in range(3):
            if piece == 0:
                wait_mine(k, 0, 0)
            if slot == 0:
                half_arrival(k, pair_first.at[k, 4 * (1 - piece)]).wait_recv()
            else:
                arrival(k, 1, pair_first.at[k, slot]).wait_recv()
            add(k, 0, *CHUNKS[0], 0, slot, 1, [], piece)
            hop(0, k, 0, *CHUNKS[0], slot, 1, piece)
    for c, group in ((2, 0), (3, 0), (0, 1), (1, 1), (2, 1), (3, 1)):
        pair_chunk(c, group)
    for k in range(3):
        load_mine(k, (0, 0))
    for c, layer, half, k in events[3:]:
        wait_mine(k, c, 0)
        if c < 3:
            arrival(k, 4 * c, pair_recv.at[k, c // 2]).wait_recv()
        add(k, c, layer, half, 0, 0, 4, [])
        hop(0, k, c, layer, half, 0, 4)
        load_mine(k, (0, c))

    def state(k, layer, half):
        here = part(k, half)
        return [
            pltpu.make_async_copy(w[k].at[layer, rows(k, 0, core, half)], out_w[k].at[layer, part(k, half, OLD)], state_sem.at[k]),
            pltpu.make_async_copy(m[k].at[layer, here], out_m[k].at[layer, here], state_sem.at[k]),
            pltpu.make_async_copy(v[k].at[layer, here], out_v[k].at[layer, here], state_sem.at[k]),
        ]

    for c, layer, half, k in events:
        if c == 0:
            arrival(k, 4 * len(CHUNKS), pair_kept.at[k]).wait_recv()
            departure(k, 8 * len(CHUNKS), pair_send.at[k]).wait_send()
            for place in CHUNKS:
                for copy in state(k, *place):
                    copy.start()
        wait_mine(k, c, 1)
        if c % 2 == 0:
            arrival(k, 8, rs_recv.at[0, k, c // 2]).wait_recv()
        add(k, c, layer, half, 1, 0, 2, [LAND1])
        hop(1, k, c, layer, half, 0, 2)
        load_mine(k, (1, c))
    for c, layer, half, k in events:
        wait_mine(k, c, 2)
        if c % 2 == 0:
            arrival(k, 4, rs_recv.at[1, k, c // 2]).wait_recv()
        add(k, c, layer, half, 2, 0, 1, [LAND1 + 2, LAND2])
        hop(2, k, c, layer, half, 0, 1)

    def adamw(k, c, layer, half):
        steps = rows_of[k] // HALVES // step_of(k)

        def body(i, _):
            here = slot_rows(k, half, 0, i)
            terms = [out_w[k][layer, slot_rows(k, half, slot, i)] for slot in (THEIRS + 7, LAND1 + 3, LAND2 + 1, LAND3)]
            terms.append(mine[k][PLACE[3, c], slot_rows(k, 0, 0, i)])
            grad = total(terms).astype(jnp.bfloat16).astype(jnp.float32)
            old = out_w[k][layer, slot_rows(k, half, OLD, i)].astype(jnp.float32)
            new_m = 0.9 * out_m[k][layer, here] + 0.1 * grad
            new_v = 0.95 * out_v[k][layer, here] + 0.05 * grad * grad
            out_m[k][layer, here] = new_m
            out_v[k][layer, here] = new_v
            new = old - 0.02 * (new_m * lax.rsqrt(new_v + 1e-8) + 0.1 * old)
            out_w[k][layer, slot_rows(k, half, me, i)] = new.astype(jnp.bfloat16)
            return 0

        lax.fori_loop(0, steps, body, 0)

    def gathered(k, c, mask):
        d1, d2, d3 = ORDERS[k]
        if not mask & d1:
            return rs_recv.at[(d3, d2, d2 ^ d3).index(mask), k, c // 2]
        return pair_first.at[k, (0, d3, d2, d2 ^ d3).index(mask ^ d1)] if c == LAST - 1 else pair_recv.at[k, c]

    def set_aside(k, layer, half, mask, target):
        start = (chip(mask) * 2 + core) * rows_of[k] + half * (rows_of[k] // HALVES)

        def body(i, _):
            there = pl.ds(pl.multiple_of(start + i * step_of(k), TILE), step_of(k))
            target[slot_rows(k, 0, 0, i)] = out_w[k][layer, there]
            return 0

        lax.fori_loop(0, rows_of[k] // HALVES // step_of(k), body, 0)

    def gather(k, c, layer, half, mask, dim):
        d = ORDERS[k][dim]
        spot = out_w[k].at[layer, rows(k, mask, core, half)]
        if dim == 0 and c == LAST:
            place = far(ORDERS[k]).index(mask)
            (target,) = [later[i].at[places.index(place)] for i, (which, places) in enumerate(CROSS) if which == k and place in places]
            set_aside(k, layer, half, mask, target)
        else:
            remote(spot, spot, ag_send.at[k], gathered(k, c, mask ^ d), at(d)).start()

    def wait_gather(k, c, mask):
        if c % 2 == 0:
            arrival(k, 2, gathered(k, c, mask)).wait_recv()

    def to_partner(k, layer, half, mask):
        spot = out_w[k].at[layer, rows(k, mask, core, half)]
        return remote(spot, spot, agp_send.at[k], pair_kept.at[k], partner)

    for first in range(0, len(CHUNKS), 2):
        two = [event for event in events if event[0] // 2 == first // 2]
        for c, layer, half, k in two:
            if c == 0:
                held = out_w[k].at[0, pl.ds(0, 10 * rows_of[k])]
                pltpu.make_async_copy(held, held, state_sem.at[k]).wait()
            wait_mine(k, c, 3)
            if c == first:
                arrival(k, 2, rs_recv.at[2, k, first // 2]).wait_recv()
                departure(k, 14, rs_sent(k, first)).wait_send()
            adamw(k, c, layer, half)
            if c > first:
                for peer in peers:
                    pl.semaphore_signal(free.at[k, first // 2], inc=1, device_id=peer, device_id_type=pl.DeviceIdType.MESH)
        for c, layer, half, k in two:
            if c == first:
                pl.semaphore_wait(free.at[k, first // 2], 4)
            for dim in (2, 1, 0):
                gather(k, c, layer, half, 0, dim)
            to_partner(k, layer, half, 0).start()

    for c, layer, half, k in events:
        d1, d2, d3 = ORDERS[k]
        wait_gather(k, c, d3)
        for dim in (1, 0):
            gather(k, c, layer, half, d3, dim)
        to_partner(k, layer, half, d3).start()
    for c, (layer, half) in enumerate(CHUNKS):
        for both in range(2):
            for k, (d1, d2, d3) in enumerate(ORDERS):
                mask = d2 ^ d3 * both
                wait_gather(k, c, mask)
                gather(k, c, layer, half, mask, 0)
                to_partner(k, layer, half, mask).start()
    for c, (layer, half) in enumerate(CHUNKS[:LAST]):
        for which in range(4):
            for k, order in enumerate(ORDERS):
                mask = order[0] ^ far(order)[which]
                if c == LAST - 1:
                    arrival(k, 1, pair_first.at[k, which]).wait_recv()
                elif which == 0:
                    arrival(k, 4, pair_recv.at[k, c]).wait_recv()
                if c == LAST - 1 and which == 3:
                    set_aside(k, layer, half, mask, hand[k])
                else:
                    to_partner(k, layer, half, mask).start()

    n = len(CHUNKS)
    for k in range(3):
        departure(k, 7 * n - 4, ag_send.at[k]).wait_send()
        departure(k, 8 * n - 5, agp_send.at[k]).wait_send()
        arrival(k, 8 * n - 5, pair_kept.at[k]).wait_recv()


def place_of(mask, size):
    me = lax.axis_index("dp")
    bits = {Z: lax.rem(lax.div(me, 2), 2), Y: lax.rem(lax.div(me, 4), 2), X: lax.div(me, 8)}
    return sum(d * ((1 - bits[d]) if mask & d else bits[d]) for d in (X, Y, Z)) * 2 * size


def put_out(*refs):
    sources, targets, sem = refs[:9], refs[9:18], refs[18]

    def put(i, layer, start, size, which):
        here = pl.ds(start, size)
        pltpu.make_async_copy(sources[i].at[layer, here], targets[i].at[layer, here], sem.at[which]).start()

    layer, half = CHUNKS[LAST]
    for k, (d1, d2, d3) in enumerate(ORDERS):
        size = sources[k].shape[1] // 16
        for j in range(4):
            put(k, 1 - layer, j * 4 * size, 4 * size, k)
        for r in (0, d3, d2, d2 ^ d3):
            put(k, layer, pl.multiple_of(place_of(r, size), TILE), 2 * size, 9 + k)
            for core in range(2):
                start = place_of(d1 ^ r, size) + core * size + (1 - half) * (size // HALVES)
                put(k, layer, pl.multiple_of(start, TILE), size // HALVES, 9 + k)
    for i in range(3, 9):
        for j in range(LAYERS):
            put(i, j, 0, sources[i].shape[1], i)
    for k in range(3):
        size = sources[k].shape[1] // 16
        for which, there in ((k, sources[k].at[0]), (9 + k, sources[k].at[0, pl.ds(0, 12 * size)])):
            pltpu.make_async_copy(there, there, sem.at[which]).wait()
    for i in range(3, 9):
        pltpu.make_async_copy(sources[i], sources[i], sem.at[i]).wait()


def put_rest(items, *refs):
    n = len(items)
    sources, out_w, sem = refs[:n], refs[n + 3 : n + 6], refs[n + 6]
    core = lax.rem(lax.axis_index("dp"), 2)
    for i, (k, c, masks, whose) in enumerate(items):
        layer, half = CHUNKS[c]
        size = sources[i].shape[-2]
        for j, mask in enumerate(masks):
            start = place_of(mask, HALVES * size) + ((1 - core if whose else core) * HALVES + half) * size
            target = out_w[k].at[layer, pl.ds(pl.multiple_of(start, TILE), size)]
            pltpu.make_async_copy(sources[i].at[j], target, sem.at[i]).start()
    for i in range(n):
        pltpu.make_async_copy(sources[i], sources[i], sem.at[i]).wait()


def solution(mesh):
    def step(*arrays):
        terms = [one.reshape(one.shape[1:]) for one in arrays[:3]]
        weights, m, v = arrays[3:6], arrays[6:9], arrays[9:12]
        blocks = [one.shape[1:] for one in m]
        n = len(CHUNKS)

        dma = pltpu.SemaphoreType.DMA
        out = pl.pallas_call(
            kernel,
            out_shape=[pltpu.VMEM(one.shape, one.dtype) for one in (*weights, *m, *v)]
            + [pltpu.VMEM((len(places), blocks[k][0] // HALVES, blocks[k][1]), jnp.bfloat16) for k, places in CROSS]
            + [pltpu.VMEM((rows // HALVES, columns), jnp.bfloat16) for rows, columns in blocks],
            in_specs=[pl.BlockSpec(memory_space=pl.ANY)] * 12,
            out_specs=[pl.BlockSpec(memory_space=pltpu.VMEM)] * (12 + len(CROSS)),
            scratch_shapes=[
                *[pltpu.VMEM((RING, rows // HALVES, columns), jnp.bfloat16) for rows, columns in blocks],
                dma((3,)),
                dma((3, 5)),
                dma((3, 2)),
                dma((3,)),
                dma((2, 3)),
                dma((3, 3, n // 2)),
                pltpu.SemaphoreType.REGULAR((3, n // 2)),
            ],
            compiler_params=pltpu.CompilerParams(collective_id=0, has_side_effects=True, vmem_limit_bytes=VMEM),
            name="step",
        )(*terms, *weights, *m, *v)
        out, later, hand = out[:9], out[9:-3], out[-3:]
        swap = [(i, i ^ 1) for i in range(16)]
        own = []
        for i, (k, _) in enumerate(CROSS):
            own.append(lax.ppermute(later[i], "dp", [(i, i ^ 2 * ORDERS[k][0]) for i in range(16)]))
        handed = []
        for k in range(3):
            handed.append(lax.ppermute(hand[k], "dp", swap)[None])
        out = pl.pallas_call(
            put_out,
            out_shape=[jax.ShapeDtypeStruct(one.shape, one.dtype) for one in (*weights, *m, *v)],
            in_specs=[pl.BlockSpec(memory_space=pl.ANY)] * 9,
            out_specs=[pl.BlockSpec(memory_space=pl.ANY)] * 9,
            scratch_shapes=[dma((12,))],
            cost_estimate=pl.CostEstimate(flops=30_000_000, bytes_accessed=48_000_000, transcendentals=0),
            compiler_params=pltpu.CompilerParams(vmem_limit_bytes=VMEM),
            name="put_out",
        )(*out)
        other = []
        for i in range(len(CROSS)):
            other.append(lax.ppermute(own[i], "dp", swap))
        arrived = {}
        for i, (k, places) in enumerate(CROSS):
            masks = tuple(ORDERS[k][0] ^ far(ORDERS[k])[place] for place in places)
            arrived[k, LAST, masks, 0], arrived[k, LAST, masks, 1] = own[i], other[i]
        for k, order in enumerate(ORDERS):
            arrived[k, LAST - 1, (order[0] ^ far(order)[3],), 1] = handed[k]
        calls = ((own[0], own[2]), (own[1], own[3], other[2], *handed), (other[0], other[1], other[3]))
        rest = [[item for item, block in arrived.items() if any(block is one for one in call)] for call in calls]
        new = out[:3]
        for items in rest:
            n = len(items)
            new = pl.pallas_call(
                functools.partial(put_rest, items),
                out_shape=[jax.ShapeDtypeStruct(one.shape, one.dtype) for one in weights],
                in_specs=[pl.BlockSpec(memory_space=pltpu.VMEM)] * n + [pl.BlockSpec(memory_space=pl.ANY)] * 3,
                out_specs=[pl.BlockSpec(memory_space=pl.ANY)] * 3,
                scratch_shapes=[dma((n,))],
                input_output_aliases={n: 0, n + 1: 1, n + 2: 2},
                cost_estimate=pl.CostEstimate(flops=3_000_000, bytes_accessed=5_000_000, transcendentals=0),
                compiler_params=pltpu.CompilerParams(vmem_limit_bytes=VMEM),
                name="put_rest",
            )(*[arrived[item] for item in items], *new)
        out = [*new, *out[3:]]
        return tuple(out)

    all_of, cut = P(None, None, None), P(None, "dp", None)
    step = jax.shard_map(
        step,
        mesh=mesh,
        in_specs=(P(("rep", "dp"), None, None, None),) * 3 + (all_of,) * 3 + (cut,) * 6,
        out_specs=(P("rep", None, None),) * 3 + (P("rep", "dp", None),) * 6,
        check_vma=False,
    )
    return step
```
